512 devices in a mesh: seq: 64 (over z, x), tp: 8 (over y, core).
Axes of the slice: x: 4, y: 4, z: 16, core: 2. Of those that a mesh axis runs over, the one named last changes fastest.
Arguments:
- mixer_input: bfloat16 [8192, 4096], P('seq', 'tp'), may hold values from -6 to 6
- gate_input: bfloat16 [8192, 4096], P('seq', 'tp'), may hold values from -6 to 6
- document_ids: int32 [8192], P('seq'), may hold values from 0 to 7, never falling along the last dimension, each value on 1 to 2048 neighbouring positions
- residual: bfloat16 [8192, 2048], P('seq'), may hold values from -6 to 6
- select_weight: bfloat16 [4096, 160], P('tp'), may hold values from -0.09375 to 0.09375
- step_weight: bfloat16 [128, 4096], P(None, 'tp'), may hold values from -0.5 to 0.5
- step_bias: float32 [4096], P('tp'), may hold values from -9 to -2.5
- decay_log: float32 [4096, 16], P('tp'), may hold values from -1.5 to 1.5
- skip_gain: float32 [4096], P('tp'), may hold values from 0.1 to 1.9
- out_weight: bfloat16 [4096, 2048], P('tp', 'seq'), may hold values from -0.09375 to 0.09375
- norm_gain: float32 [2048], replicated, may hold values from 0.1 to 1.9
- project_weight: bfloat16 [2048, 3, 2048], P('seq', None, 'tp'), may hold values from -4 to 4
Outputs:
- attention: bfloat16 [8192, 2048], P('seq', 'tp')
The draws below stay inside these ranges and needn't reach their ends.
Inputs may be any that keep to these rules, and one draw needn't show every extreme that they name: `document_ids`: ids never fall along the sequence; every document has 1 to 2048 tokens.
All inputs are finite; a program needn't handle non-finite values.
Results may differ from the reference program's by a relative error of at most 0.02.
Values may be sent and summed in bfloat16 or wider, within the bound.
A program may use at most 64 MiB of HBM per device.

```python
import math
import jax
import jax.numpy as jnp
import numpy as np
from jax import lax

D = 2048
DI = 4096
STATE = 16
RANK = 128
HEADS = 16
HEAD = 128
WINDOW = 2048
TOK_DEV = 128
LENGTH = 8192
DOCS = 8
DOC_MOST = 2048


def draw_project_weight(key, part):
    first_key = jax.random.fold_in(jax.random.fold_in(key, 7301), 0)
    second_key = jax.random.fold_in(jax.random.fold_in(key, 7301), 1)
    fourth_key = jax.random.fold_in(jax.random.fold_in(key, 7301), 3)
    spread = D ** (-0.5)
    key_weight = jax.random.normal(first_key, (D, HEADS * HEAD), jnp.float32) * spread
    value_weight = jax.random.normal(second_key, (D, HEADS * HEAD), jnp.float32) * spread
    query_weight = jax.random.normal(fourth_key, (D, HEADS * HEAD), jnp.float32) * spread
    stacked = jnp.stack([query_weight, key_weight, value_weight], axis=1)
    return jnp.clip(stacked, -4.0, 4.0).astype(jnp.bfloat16)


def levels(stream_key, dims, cuts, low, high):
    def one(dim, parts):
        draws = jax.random.uniform(jax.random.fold_in(jax.random.fold_in(stream_key, 6), dim), (parts,), jnp.float32, low / len(cuts), high / len(cuts))
        return jnp.repeat(jnp.exp(draws), dims[dim] // parts).reshape((-1,) + (1,) * (len(dims) - dim - 1))

    loudness = one(*cuts[0])
    for cut in cuts[1:]:
        loudness = loudness * one(*cut)
    return loudness


def profile(count, total, limit, slope):
    portions = [(1 << 20) // math.isqrt(grade ** slope) + 1 for grade in range(2, count + 1)]
    surplus, given = total - limit - (count - 1), [1] * (count - 1)
    while surplus > 0:
        candidates = [i for i in range(count - 1) if given[i] < limit]
        mass, left = sum([portions[i] for i in candidates]), surplus
        for i in candidates:
            addition = min(limit - given[i], max(1, left * portions[i] // mass), surplus)
            given[i] = given[i] + addition
            surplus = surplus - addition
    return np.array([limit] + given)


def ragged_sizes(key, number_of, total, most, skew):
    if number_of == 2:
        one = jax.random.randint(key, (), max(1, total - most), min(most, total - 1) + 1)
        return jnp.stack([one, total - one])
    tallies = jnp.asarray(profile(number_of, total, most, skew), jnp.int32)
    pairs = (number_of - 1) // 2
    donor, taker = tallies[1:1 + 2 * pairs:2], tallies[2:2 + 2 * pairs:2]
    room = jnp.minimum(donor - 1, most - taker)
    shifted = jax.random.randint(jax.random.fold_in(key, 1), (pairs,), 0, 1 << 20) % (room + 1)
    tallies = tallies.at[1:1 + 2 * pairs:2].set(donor - shifted).at[2:2 + 2 * pairs:2].set(taker + shifted)
    return tallies[jax.random.permutation(jax.random.fold_in(key, 2), number_of)]


def normal_values(own_key, dims, scale, most, pieces=(), kind=jnp.bfloat16):
    drawn = jax.random.normal(own_key, dims, jnp.float32) * scale
    if len(pieces) > 0:
        drawn = levels(own_key, dims, pieces, -0.22, 0.18) * drawn
    return jnp.clip(drawn, min=-most, max=most).astype(kind)


def setup_inputs(seed: int = 0) -> dict:
    streams_of = jax.random.split(jax.random.key(seed), 13)
    return {
        "mixer_input": normal_values(streams_of[0], (LENGTH, DI), 1.0, 6.0, ((0, 64), (1, 8))),
        "gate_input": normal_values(streams_of[1], (LENGTH, DI), 1.0, 6.0, ((0, 64), (1, 8))),
        "document_ids": jnp.searchsorted(jnp.cumsum(ragged_sizes(streams_of[2], DOCS, LENGTH, DOC_MOST, 1)), jnp.arange(LENGTH), side="right").astype(jnp.int32),
        "residual": normal_values(streams_of[3], (LENGTH, D), 1.0, 6.0, ((0, 64),)),
        "select_weight": normal_values(streams_of[4], (DI, RANK + 2 * STATE), DI ** -0.5, 0.09375, ((0, 8),)),
        "step_weight": normal_values(streams_of[5], (RANK, DI), RANK ** -0.5, 0.5, ((1, 8),)),
        "step_bias": jnp.clip(-9.0 + 6.5 * jax.random.uniform(streams_of[6], (DI,), jnp.float32) ** levels(streams_of[6], (DI,), ((0, 8),), -0.2, 0.2), -9.0, -2.5),
        "decay_log": jnp.clip(jax.random.uniform(streams_of[7], (DI, STATE), jnp.float32, -1.5, 1.5) * levels(streams_of[7], (DI, STATE), ((0, 8),), -0.4, 0.0), -1.5, 1.5),
        "skip_gain": jnp.clip(1.0 + 0.18 * jax.random.normal(streams_of[8], (DI,), jnp.float32), 0.1, 1.9),
        "out_weight": normal_values(streams_of[9], (DI, D), DI ** -0.5, 0.09375, ((0, 8), (1, 64))),
        "norm_gain": jnp.clip(1.0 + 0.18 * jax.random.normal(streams_of[10], (D,), jnp.float32), 0.1, 1.9),
        "project_weight": draw_project_weight(jax.random.fold_in(streams_of[12], 71), 0),
    }


norm_eps = 1e-05

def selective_scan(initial, step_size, input_coef, output_coef, values, keep_flags, decay_rate):

    def advance(carried, inputs):
        step_row, input_row, output_row, value_row, keep_row = inputs
        carried = jnp.exp(step_row[:, None] * decay_rate) * carried * keep_row + (step_row * value_row)[:, None] * input_row[None, :]
        return (carried, lax.optimization_barrier(jnp.sum(carried * output_row[None, :], axis=1)))
    return lax.scan(advance, initial, (step_size, input_coef, output_coef, values, keep_flags))

def scale_rows(stream, norm_gain):
    widened = stream.astype(jnp.float32)
    return (widened * lax.rsqrt(lax.optimization_barrier(jnp.mean(widened * widened, axis=-1, keepdims=True)) + norm_eps) * norm_gain).astype(jnp.bfloat16)

def reference(mixer_input, gate_input, document_ids, residual, select_weight, step_weight, step_bias, decay_log, skip_gain, out_weight, norm_gain, project_weight):
    total_rows = mixer_input.shape[0]
    selected = jnp.dot(mixer_input, select_weight, preferred_element_type=jnp.float32)
    step_low = selected[:, :RANK].astype(jnp.bfloat16)
    input_coef = selected[:, RANK:RANK + STATE]
    output_coef = selected[:, RANK + STATE:]
    step_size = jax.nn.softplus(jnp.dot(step_low, step_weight, preferred_element_type=jnp.float32) + step_bias)
    decay_rate = -jnp.exp(decay_log)
    values = mixer_input.astype(jnp.float32)
    same_document = document_ids[1:] == document_ids[:-1]
    keep_flags = jnp.concatenate([jnp.zeros((1,), jnp.float32), same_document.astype(jnp.float32)])
    initial = jnp.zeros((DI, STATE), jnp.float32)
    final_state, scanned = selective_scan(initial, step_size, input_coef, output_coef, values, keep_flags, decay_rate)
    gated = ((scanned + skip_gain * values) * jax.nn.silu(gate_input.astype(jnp.float32))).astype(jnp.bfloat16)
    stream = (jnp.dot(gated, out_weight, preferred_element_type=jnp.float32) + residual.astype(jnp.float32)).astype(jnp.bfloat16)
    normed = scale_rows(stream, norm_gain)
    triples = jnp.dot(normed, project_weight.reshape(D, 3 * HEADS * HEAD), preferred_element_type=jnp.float32)
    triples = triples.astype(jnp.bfloat16).reshape(total_rows, 3, HEADS, HEAD)
    position = jnp.arange(total_rows, dtype=jnp.int32)
    start_flags = jnp.concatenate([jnp.ones((1,), bool), jnp.logical_not(same_document)])
    document_start = lax.cummax(jnp.where(start_flags, position, jnp.zeros_like(position)))
    padding = jnp.zeros((WINDOW, HEADS, HEAD), jnp.bfloat16)
    keys_padded = jnp.concatenate([padding, triples[:, 1]], axis=0)
    values_padded = jnp.concatenate([padding, triples[:, 2]], axis=0)
    queries_all = triples[:, 0]
    block_rows = TOK_DEV

    def attend(block_index):
        first_row = block_index * block_rows
        queries = lax.dynamic_slice_in_dim(queries_all, first_row, block_rows, 0)
        key_rows = lax.dynamic_slice_in_dim(keys_padded, first_row, WINDOW + block_rows, 0)
        value_rows = lax.dynamic_slice_in_dim(values_padded, first_row, WINDOW + block_rows, 0)
        query_position = first_row + jnp.arange(block_rows, dtype=jnp.int32)
        key_position = first_row - WINDOW + jnp.arange(WINDOW + block_rows, dtype=jnp.int32)
        starts_here = lax.dynamic_slice_in_dim(document_start, first_row, block_rows, 0)
        scores = jnp.einsum('qhd,khd->hqk', queries.astype(jnp.float32), key_rows.astype(jnp.float32)) * HEAD ** (-0.5)
        allowed = (key_position[None, :] <= query_position[:, None]) & (key_position[None, :] > query_position[:, None] - WINDOW) & (key_position[None, :] >= starts_here[:, None])
        masked = jnp.where(allowed[None], scores, -jnp.inf)
        row_max = lax.optimization_barrier(jnp.max(masked, axis=-1, keepdims=True))
        weights = jnp.where(allowed[None], jnp.exp(scores - row_max), 0.0)
        weights = (weights / lax.optimization_barrier(jnp.sum(weights, axis=-1, keepdims=True))).astype(jnp.bfloat16)
        mixed = jnp.einsum('hqk,khd->qhd', weights.astype(jnp.float32), value_rows.astype(jnp.float32))
        return mixed.astype(jnp.bfloat16).reshape(block_rows, HEADS * HEAD)
    blocks = lax.map(attend, jnp.arange(total_rows // block_rows, dtype=jnp.int32))
    return blocks.reshape(total_rows, HEADS * HEAD)
```

```python
import jax
import jax.numpy as jnp
from jax import lax
from jax.experimental import pallas as pl
from jax.experimental.pallas import tpu as pltpu
from jax.sharding import Mesh
from jax.sharding import PartitionSpec as P

MESH = pl.DeviceIdType.MESH
NZ, NX, NY, NC = 16, 4, 4, 2
STATE = 16
RANK = 128
HEAD = 128
WINDOW = 2048
EPS = 1e-05
LOG2E = 1.4426950408889634
RESET = 1e6
HIDDEN = -1e30
SEQ = ("z", "x")
TP = ("y", "c")
F32 = jnp.float32
BF16 = jnp.bfloat16


def nt(a, b):
    return lax.dot_general(a, b, (((1,), (1,)), ((), ())), preferred_element_type=F32)


def nn(a, b):
    return jnp.dot(a, b, preferred_element_type=F32)


def iota(shape, dim):
    return lax.broadcasted_iota(jnp.int32, shape, dim)


def softplus(v):
    e = jnp.exp(-jnp.abs(v))
    small = e * (1.0 - e * (0.5 - e * (1.0 / 3.0 - e * 0.25)))
    return jnp.maximum(v, 0.0) + jnp.where(e < 0.01, small, jnp.log(1.0 + e))


class Links:
    def __init__(self, send, recv):
        self.send, self.recv = send, recv
        self.sends, self.recvs = 0, 0
        self.open = []

    def slots(self, count):
        first = self.recvs
        self.recvs += count
        return first

    def copy(self, src, dst, device, slot, send=None):
        if send is None:
            send = self.sends
            self.sends += 1
        return pltpu.make_async_remote_copy(
            src_ref=src,
            dst_ref=dst,
            send_sem=self.send.at[send],
            recv_sem=self.recv.at[slot],
            device_id=device,
            device_id_type=MESH,
        )

    def start(self, src, dst, device, slot):
        made = self.copy(src, dst, device, slot)
        made.start()
        self.open.append(made)

    def wait(self, dst, slot, device):
        self.copy(dst, dst, device, slot, 0).wait_recv()

    def drain(self):
        for made in self.open:
            made.wait_send()


def kernel(
    x_ref, g_ref, ids_ref, res_ref, sel_ref, stepw_ref, bias_ref, a_ref, skip_ref, wo_ref, gain_ref, wp_ref,
    out_ref,
    part, rs1, sb, ids, dt2, bx, hb, hs, ss, hz, sz, hr, sr, xw, wp, ys, gt, ps, pr, ow, r2s, r2, na, nb,
    kv, qd, ob, outb, send_sem, recv_sem,
):
    z, x, y, c = (lax.axis_index(n) for n in ("z", "x", "y", "c"))
    other = 1 - c

    def zat(d):
        return lax.rem(z + d + NZ, NZ)

    def xat(d):
        return lax.rem(x + d, NX)

    def yat(d):
        return lax.rem(y + d, NY)

    def cat(d):
        return other if d else c

    peers = [(z, x, yat(dy), cat(dc)) for dy in range(NY) for dc in range(NC) if dy or dc]
    row_peers = [(z, xat(dx), y, cat(dc)) for dx in range(1, NX) for dc in range(NC)]
    far = [(zat(d), x, y, c) for d in (-4, -3, -2, -1, 1, 2, 3, 4)]
    barrier = pltpu.get_barrier_semaphore()
    everyone = peers + row_peers + far
    for device in everyone:
        pl.semaphore_signal(barrier, inc=1, device_id=device, device_id_type=MESH)

    links = Links(send_sem, recv_sem)
    me = (z, x, y, c)
    partner = (z, x, y, other)
    my_rows = pl.multiple_of(64 * c + 16 * y, 16)

    part[...] = nn(x_ref[...], sel_ref[...])
    xw[z, x] = wo_ref[...]
    ids[0, :, pl.ds(pl.multiple_of(128 * x, 128), 128)] = ids_ref[...]
    pl.semaphore_wait(barrier, len(everyone))

    slot_rs = links.slots(8)
    for dy in range(NY):
        for dc in range(NC):
            if dy or dc:
                ty, tc = yat(dy), cat(dc)
                rows = pl.multiple_of(64 * tc + 16 * ty, 16)
                links.start(part.at[pl.ds(rows, 16)], rs1.at[dy * 2 + dc], (z, x, ty, tc), slot_rs + dy * 2 + dc)

    slot_x0 = links.slots(2)
    for hh in range(2):
        links.start(wp_ref.at[hh], wp.at[z, x], (z, 2 * c + hh, y, 1 - x // 2), slot_x0 + lax.rem(x, 2))
    slot_i1 = links.slots(4)
    row_part = pl.ds(pl.multiple_of(128 * x, 128), 128)
    for dx in range(1, NX):
        links.start(ids_ref, ids.at[0, :, row_part], (z, xat(dx), y, c), slot_i1 + dx)

    slot_wo = {d: links.slots(1) for d in (-7, -6, -5, -4, -3, -2, -1, 1, 2, 3, 4, 5, 6, 7, 8)}
    slot_wp = {d: links.slots(1) for d in (-7, -6, -5, -4, -3, -2, -1, 1, 2, 3, 4, 5, 6, 7, 8)}
    ringed = pl.ds(pl.multiple_of(2 * other, 2), 2)

    def hops(phase):
        right = [2 * phase - 1, 2 * phase]
        left = [-d for d in right if d < 8]
        return right + left

    def ring_out(phase):
        for sign in (1, -1):
            block = zat(-sign * 2 * (phase - 1))
            for near in (1, 2):
                far_by = sign * (2 * (phase - 1) + near)
                if far_by != -8:
                    links.start(
                        wo_ref if phase == 1 else xw.at[block, x],
                        xw.at[block, x],
                        (zat(sign * near), x, y, c),
                        slot_wo[far_by],
                    )

    def ring_proj(phase):
        for sign in (1, -1):
            block = zat(-sign * 2 * (phase - 1))
            for near in (1, 2):
                far_by = sign * (2 * (phase - 1) + near)
                if far_by != -8:
                    links.start(
                        wp.at[block, ringed],
                        wp.at[block, ringed],
                        (zat(sign * near), x, y, c),
                        slot_wp[far_by],
                    )

    def ring_wait(phase, slots, at):
        for d in hops(phase):
            links.wait(at(zat(-d)), slots[d], (zat(1 if d > 0 else -1), x, y, c))

    def wo_at(block):
        return xw.at[block, x]

    def wp_at(block):
        return wp.at[block, ringed]

    slot_xw = links.slots(4)
    first_xw = links.sends
    links.sends += 3

    def spread(blocks):
        for block in blocks:
            for dx in range(1, NX):
                links.copy(
                    xw.at[block, x], xw.at[block, x], (z, xat(dx), y, c), slot_xw + dx, first_xw + dx - 1
                ).start()

    ring_out(1)

    total = part[pl.ds(my_rows, 16), :]
    for k in range(1, 8):
        links.wait(rs1.at[k], slot_rs + k, partner)
        total = total + rs1[k]
    sb[pl.ds(my_rows, 16), :] = total.astype(BF16)
    slot_ag = links.slots(8)
    for dy in range(NY):
        for dc in range(NC):
            if dy or dc:
                mine = sb.at[pl.ds(my_rows, 16)]
                links.start(mine, mine, (z, x, yat(dy), cat(dc)), slot_ag + dy * 2 + dc)

    for dx in range(1, NX):
        links.wait(ids.at[0, :, row_part], slot_i1 + dx, (z, xat(dx), y, c))
    slot_i2 = links.slots(5)
    for dz in range(1, 5):
        links.start(ids.at[0], ids.at[dz], (zat(dz), x, y, c), slot_i2 + dz)
    for k in range(2):
        links.wait(wp.at[z, x], slot_x0 + k, partner)
    ring_proj(1)

    for k in range(1, 8):
        links.wait(sb.at[pl.ds(my_rows, 16)], slot_ag + k, partner)
    for dz in range(1, 5):
        links.wait(ids.at[dz], slot_i2 + dz, (zat(dz), x, y, c))

    values = x_ref[...].astype(F32)
    step = softplus(nn(sb[:, :RANK], stepw_ref[...]) + bias_ref[...])
    last = [jnp.broadcast_to(ids[0, :, 128 * k + 127 : 128 * k + 128], (1, 128)) for k in range(NX)]
    prior = jnp.broadcast_to(ids[1, :, 511:512], (1, 128))
    prior = jnp.where(z == 0, jnp.full_like(prior, -1.0), prior)
    for k in range(1, NX):
        prior = jnp.where(x == k, last[k - 1], prior)
    column = jnp.transpose(jnp.broadcast_to(ids_ref[...], (128, 128)))
    before = pltpu.roll(column, 1, axis=0)
    before = jnp.where(iota((128, 128), 0) == 0, jnp.broadcast_to(prior, (128, 128)), before)
    linked = column == before
    for k in range(4):
        cols = slice(128 * k, 128 * k + 128)
        dt2[:, cols] = jnp.where(linked, step[:, cols], RESET)
    ss[x] = jnp.sum(dt2[...], axis=0, keepdims=True)
    slot_ss = links.slots(4)
    for dx in range(1, NX):
        links.start(ss.at[x], ss.at[x], (z, xat(dx), y, c), slot_ss + dx)

    driven = (step * values).astype(BF16)
    pick = (lax.rem(iota((256, 128), 0), STATE) == iota((256, 128), 1)).astype(BF16)
    inputs = nt(pick, sb[:, RANK:])

    def fill(k, _):
        token = iota((256, 128), 0) // STATE + k * 16
        spread_in = jnp.where(iota((256, 128), 1) == token, inputs, 0.0).astype(BF16)
        bx[pl.ds(pl.multiple_of(k * 256, 256), 256), :] = nn(spread_in, driven)
        return 0

    lax.fori_loop(0, 8, fill, 0)
    rate = a_ref[...]

    def scan(initial, keep_states):
        def advance(k, h):
            steps = dt2[pl.ds(pl.multiple_of(k * 8, 8), 8), :]
            for j in range(8):
                at = pl.ds(pl.multiple_of(k * 128 + j * 16, 16), 16)
                h = jnp.exp2(rate * steps[j : j + 1, :]) * h + bx[at, :]
                if keep_states:
                    hb[at, :] = h.astype(BF16)
            return h

        return lax.fori_loop(0, 16, advance, initial)

    hs[x] = scan(jnp.zeros((STATE, 512), F32), False).astype(BF16)
    slot_hs = links.slots(4)
    for dx in range(1, NX):
        links.start(hs.at[x], hs.at[x], (z, xat(dx), y, c), slot_hs + dx)
    ring_wait(1, slot_wo, wo_at)
    ring_out(2)
    ring_wait(1, slot_wp, wp_at)
    ring_proj(2)

    for dx in range(1, NX):
        links.wait(ss.at[x], slot_ss + dx, (z, xat(dx), y, c))
        links.wait(hs.at[x], slot_hs + dx, (z, xat(dx), y, c))
    running = jnp.zeros((STATE, 512), F32)
    steps_sum = jnp.zeros((1, 512), F32)
    own_prior, own_steps = running, steps_sum
    for k in range(NX):
        own_prior = jnp.where(x == k, running, own_prior)
        own_steps = jnp.where(x == k, steps_sum, own_steps)
        running = jnp.exp2(rate * ss[k]) * running + hs[k].astype(F32)
        steps_sum = steps_sum + ss[k]
    hr[...] = running.astype(BF16)
    sr[...] = steps_sum
    slot_hz, slot_sz = links.slots(5), links.slots(5)
    for dz in range(1, 5):
        links.start(hr, hz.at[dz - 1], (zat(dz), x, y, c), slot_hz + dz)
        links.start(sr, sz.at[dz - 1], (zat(dz), x, y, c), slot_sz + dz)
    spread([z] + [zat(-d) for d in hops(1)])
    ring_wait(2, slot_wo, wo_at)
    ring_out(3)
    spread([zat(-d) for d in hops(2)])
    for dz in range(1, 5):
        links.wait(hz.at[dz - 1], slot_hz + dz, (zat(dz), x, y, c))
        links.wait(sz.at[dz - 1], slot_sz + dz, (zat(dz), x, y, c))
    above = jnp.zeros((STATE, 512), F32)
    for dz in range(4, 0, -1):
        joined = jnp.exp2(rate * sz[dz - 1]) * above + hz[dz - 1].astype(F32)
        above = jnp.where(z >= dz, joined, jnp.zeros_like(joined))
    carry = jnp.exp2(rate * own_steps) * above + own_prior
    ring_wait(2, slot_wp, wp_at)
    ring_proj(3)
    scan(carry, True)
    ring_wait(3, slot_wo, wo_at)
    ring_out(4)
    spread([zat(-d) for d in hops(3)])
    ring_wait(3, slot_wp, wp_at)
    ring_proj(4)

    pick_out = (lax.rem(iota((256, 128), 0), STATE) + STATE == iota((256, 128), 1)).astype(BF16)
    own_token = iota((16, 256), 1) // STATE == iota((16, 256), 0)

    def contract(k, _):
        rows = pl.ds(pl.multiple_of(k * 16, 16), 16)
        coef = nt(sb[rows, RANK:], pick_out)
        coef = jnp.where(own_token, coef, 0.0).astype(BF16)
        ys[rows, :] = nn(coef, hb[pl.ds(pl.multiple_of(k * 256, 256), 256), :])
        return 0

    lax.fori_loop(0, 8, contract, 0)
    gate = g_ref[...].astype(F32)
    mixed = (ys[...] + skip_ref[...] * values) * (gate / (1.0 + jnp.exp(-gate)))
    gt[...] = mixed.astype(BF16)

    ring_wait(4, slot_wo, wo_at)
    spread([zat(-d) for d in hops(4)])
    for dx in range(1, NX):
        links.wait(xw.at[:, x], slot_xw + dx, (z, xat(dx), y, c))

    def project(target, half, extra):
        rows = pl.ds(pl.multiple_of(64 * half, 64), 64)

        def one(k, _):
            weight = xw[pl.ds(2 * k, 2)].reshape(256, 512)
            product = nt(gt[rows, :], weight)
            cols = pl.ds(pl.multiple_of(k * 256, 256), 256)
            if extra is not None:
                product = product + extra[:, cols].astype(F32)
            target[:, cols] = product.astype(target.dtype)
            return 0

        lax.fori_loop(0, 8, one, 0)

    project(ps, other, None)
    slot_pr = links.slots(1)
    links.start(ps, pr, partner, slot_pr)
    ring_wait(4, slot_wp, wp_at)
    slot_pw = links.slots(1)
    links.start(wp.at[:, ringed], wp.at[:, ringed], partner, slot_pw)
    links.wait(pr, slot_pr, partner)
    project(ow, c, pr)
    r2s[...] = ow[...].astype(BF16)
    slot_r2 = links.slots(4)
    for dy in range(1, NY):
        ty = yat(dy)
        links.start(r2s.at[pl.ds(pl.multiple_of(16 * ty, 16), 16)], r2.at[dy], (z, x, ty, c), slot_r2 + dy)
    stream = ow[pl.ds(pl.multiple_of(16 * y, 16), 16), :] + res_ref[pl.ds(my_rows, 16), :].astype(F32)
    for dy in range(1, NY):
        links.wait(r2.at[dy], slot_r2 + dy, partner)
        stream = stream + r2[dy].astype(F32)
    stream = stream.astype(BF16).astype(F32)
    normed = stream * lax.rsqrt(jnp.mean(stream * stream, axis=-1, keepdims=True) + EPS) * gain_ref[...]
    normed = normed.astype(BF16)

    na[x, y] = normed[:, :1024]
    nb[x, y] = normed[:, 1024:]
    slot_n1, slot_n2, slot_n3, slot_n4 = (links.slots(4) for _ in range(4))
    for d in range(1, 4):
        links.start(na.at[x, y], na.at[x, y], (z, xat(d), y, c), slot_n1 + d)
        links.start(nb.at[x, y], nb.at[x, y], (z, x, yat(d), c), slot_n2 + d)
    for d in range(1, 4):
        links.wait(na.at[x, y], slot_n1 + d, partner)
    for d in range(1, 4):
        links.start(na.at[:, y], na.at[:, y], (z, x, yat(d), c), slot_n3 + d)
    for d in range(1, 4):
        links.wait(nb.at[x, y], slot_n2 + d, partner)
    for d in range(1, 4):
        links.start(nb.at[x], nb.at[x], (z, xat(d), y, c), slot_n4 + d)

    for k in range(NX):
        qd[k] = jnp.transpose(jnp.broadcast_to(ids[0, :, 128 * k : 128 * k + 128], (128, 128)))
    half_rows = pl.ds(pl.multiple_of(64 * c, 64), 64)
    q_doc = jnp.concatenate([qd[k, half_rows, :] for k in range(NX)], axis=0)
    q_doc = jnp.concatenate([q_doc] * 4, axis=1)
    row_of = iota((256, 512), 0)
    q_pos = 512 * z + 128 * (row_of // 64) + 64 * c + lax.rem(row_of, 64)

    links.wait(wp.at[:, ringed], slot_pw, partner)
    for d in range(1, 4):
        links.wait(na.at[:, y], slot_n3 + d, partner)
    for d in range(1, 4):
        links.wait(nb.at[x], slot_n4 + d, partner)
    triple = nn(na[...].reshape(256, 1024), wp[0:8].reshape(1024, 384))
    triple = triple + nn(nb[...].reshape(256, 1024), wp[8:16].reshape(1024, 384))
    query = triple[:, :HEAD].astype(BF16)
    kv[0, :, c] = triple[:, HEAD:].astype(BF16).reshape(4, 64, 256)

    slot_kz = [links.slots(2) for _ in range(5)]
    slot_kc = [links.slots(2) for _ in range(5)]

    def chunk(d, part_of, core):
        return kv.at[d, pl.ds(2 * part_of, 2), core]

    def pass_on(d, part_of):
        if d < 4:
            links.start(chunk(d, part_of, c), chunk(d + 1, part_of, c), (zat(1), x, y, c), slot_kz[d + 1] + part_of)
        links.start(chunk(d, part_of, c), chunk(d, part_of, c), partner, slot_kc[d] + part_of)

    top = jnp.full((256, 1), HIDDEN, F32)
    mass = jnp.zeros((256, 1), F32)
    acc = jnp.zeros((256, HEAD), F32)

    def attend(d, carried):
        top, mass, acc = carried
        for p in range(2):
            links.wait(chunk(d, p, other), slot_kc[d] + p, partner)
        block = kv[d].reshape(512, 256)
        scores = nt(query, block[:, :HEAD]) * HEAD**-0.5
        k_pos = 512 * (z - d) + iota((256, 512), 1)
        k_doc = jnp.broadcast_to(ids[d], (256, 512))
        allowed = (k_pos >= 0) & (k_pos <= q_pos) & (k_pos > q_pos - WINDOW) & (k_doc == q_doc)
        scores = jnp.where(allowed, scores, HIDDEN)
        new_top = jnp.maximum(top, jnp.max(scores, axis=-1, keepdims=True))
        probs = jnp.exp(scores - new_top)
        shrink = jnp.exp(top - new_top)
        mass = mass * shrink + jnp.sum(probs, axis=-1, keepdims=True)
        acc = acc * shrink + nn(probs.astype(BF16), block[:, HEAD:])
        return new_top, mass, acc

    carried = (top, mass, acc)
    for p in range(2):
        pass_on(0, p)
    for d in range(1, 5):
        for p in range(2):
            links.wait(chunk(d, p, c), slot_kz[d] + p, partner)
            pass_on(d, p)
        carried = attend(d - 1, carried)
    top, mass, acc = attend(4, carried)
    ob[...] = (acc / mass).astype(BF16).reshape(4, 64, HEAD)

    slot_o = links.slots(4)
    mine = slot_o + lax.rem(x, 2) * 2 + c
    cols = pl.ds(pl.multiple_of(128 * lax.rem(x, 2), 128), 128)
    for dx in range(1, NX):
        tx = xat(dx)
        links.start(ob.at[tx], outb.at[half_rows, cols], (z, tx, y, x // 2), mine)
    stays = c == x // 2
    to_partner = links.copy(ob.at[x], outb.at[half_rows, cols], partner, mine)

    @pl.when(stays)
    def _():
        outb[half_rows, cols] = ob[x]

    @pl.when(jnp.logical_not(stays))
    def _():
        to_partner.start()

    for k in range(4):
        from_me = stays & (lax.rem(x, 2) * 2 + c == k)

        @pl.when(jnp.logical_not(from_me))
        def _():
            links.wait(outb.at[half_rows, cols], slot_o + k, partner)

    out_ref[...] = outb[...]

    @pl.when(jnp.logical_not(stays))
    def _():
        to_partner.wait_send()

    links.drain()
    for dx in range(1, NX):
        links.copy(xw.at[:, x], xw.at[:, x], (z, xat(dx), y, c), slot_xw + dx, first_xw + dx - 1).wait_send()
    assert links.sends <= SENDS and links.recvs <= RECVS, (links.sends, links.recvs)


SENDS, RECVS = 160, 160


def body(
    mixer_input, gate_input, document_ids, residual, select_weight, step_weight, step_bias, decay_log, skip_gain,
    out_weight, norm_gain, project_weight,
):
    vmem = pl.BlockSpec(memory_space=pltpu.VMEM)
    operands = (
        mixer_input,
        gate_input,
        document_ids.astype(F32).reshape(1, 128),
        residual,
        jnp.pad(select_weight, ((0, 0), (0, 96))),
        step_weight,
        step_bias.reshape(1, 512),
        -jnp.exp(decay_log).T * LOG2E,
        skip_gain.reshape(1, 512),
        out_weight.T,
        norm_gain.reshape(1, 2048),
        project_weight.reshape(32, 3, 2, 128).transpose(2, 0, 1, 3).reshape(2, 32, 384),
    )
    scratch = [
        pltpu.VMEM((128, 256), F32),
        pltpu.VMEM((8, 16, 256), F32),
        pltpu.VMEM((128, 256), BF16),
        pltpu.VMEM((5, 1, 512), F32),
        pltpu.VMEM((128, 512), F32),
        pltpu.VMEM((2048, 512), F32),
        pltpu.VMEM((2048, 512), BF16),
        pltpu.VMEM((4, 16, 512), BF16),
        pltpu.VMEM((4, 1, 512), F32),
        pltpu.VMEM((4, 16, 512), BF16),
        pltpu.VMEM((4, 1, 512), F32),
        pltpu.VMEM((16, 512), BF16),
        pltpu.VMEM((1, 512), F32),
        pltpu.VMEM((16, 4, 32, 512), BF16),
        pltpu.VMEM((16, 4, 32, 384), BF16),
        pltpu.VMEM((128, 512), F32),
        pltpu.VMEM((128, 512), BF16),
        pltpu.VMEM((64, 2048), BF16),
        pltpu.VMEM((64, 2048), BF16),
        pltpu.VMEM((64, 2048), F32),
        pltpu.VMEM((64, 2048), BF16),
        pltpu.VMEM((4, 16, 2048), BF16),
        pltpu.VMEM((4, 4, 16, 1024), BF16),
        pltpu.VMEM((4, 4, 16, 1024), BF16),
        pltpu.VMEM((5, 4, 2, 64, 256), BF16),
        pltpu.VMEM((4, 128, 128), F32),
        pltpu.VMEM((4, 64, 128), BF16),
        pltpu.VMEM((128, 256), BF16),
        pltpu.SemaphoreType.DMA((SENDS,)),
        pltpu.SemaphoreType.DMA((RECVS,)),
    ]
    return pl.pallas_call(
        kernel,
        out_shape=jax.ShapeDtypeStruct((128, 256), BF16),
        in_specs=[vmem] * len(operands),
        out_specs=vmem,
        scratch_shapes=scratch,
        compiler_params=pltpu.CompilerParams(collective_id=0, has_side_effects=True, vmem_limit_bytes=48 << 20),
    )(*operands)


def solution(mesh):
    split = Mesh(mesh.devices.reshape(NZ, NX, NY, NC), ("z", "x", "y", "c"))
    placed = (
        P(SEQ, TP), P(SEQ, TP), P(SEQ), P(SEQ, None), P(TP, None), P(None, TP), P(TP), P(TP, None), P(TP),
        P(TP, SEQ), P(), P(SEQ, None, TP),
    )
    return jax.shard_map(body, mesh=split, in_specs=placed, out_specs=P(SEQ, TP), check_vma=False)
```

```python
import jax
import jax.numpy as jnp
from jax import lax
from jax.experimental import pallas as pl
from jax.experimental.pallas import tpu as pltpu
from jax.sharding import Mesh
from jax.sharding import PartitionSpec as P

MESH = pl.DeviceIdType.MESH
NZ, NX, NY, NC = 16, 4, 4, 2
STATE = 16
RANK = 128
HEAD = 128
WINDOW = 2048
EPS = 1e-05
LOG2E = 1.4426950408889634
RESET = 1e6
HIDDEN = -1e30
SEQ = ("z", "x")
TP = ("y", "c")
F32 = jnp.float32
BF16 = jnp.bfloat16


def nt(a, b):
    return lax.dot_general(a, b, (((1,), (1,)), ((), ())), preferred_element_type=F32)


def nn(a, b):
    return jnp.dot(a, b, preferred_element_type=F32)


def iota(shape, dim):
    return lax.broadcasted_iota(jnp.int32, shape, dim)


def softplus(v):
    e = jnp.exp(-jnp.abs(v))
    small = e * (1.0 - e * (0.5 - e * (1.0 / 3.0 - e * 0.25)))
    return jnp.maximum(v, 0.0) + jnp.where(e < 0.01, small, jnp.log(1.0 + e))


class Links:
    def __init__(self, send, recv):
        self.send, self.recv = send, recv
        self.sends, self.recvs = 0, 0
        self.open = []

    def slots(self, count):
        first = self.recvs
        self.recvs += count
        return first

    def copy(self, src, dst, device, slot, send=None):
        if send is None:
            send = self.sends
            self.sends += 1
        return pltpu.make_async_remote_copy(
            src_ref=src,
            dst_ref=dst,
            send_sem=self.send.at[send],
            recv_sem=self.recv.at[slot],
            device_id=device,
            device_id_type=MESH,
        )

    def start(self, src, dst, device, slot):
        made = self.copy(src, dst, device, slot)
        made.start()
        self.open.append(made)

    def wait(self, dst, slot, device):
        self.copy(dst, dst, device, slot, 0).wait_recv()

    def drain(self):
        for made in self.open:
            made.wait_send()


def kernel(
    x_ref, g_ref, ids_ref, res_ref, sel_ref, stepw_ref, bias_ref, a_ref, skip_ref, wo_ref, gain_ref, wp_ref,
    out_ref,
    part, part16, rs1, sb, ids, dt2, bx, hb, hs, ss, hz, sz, hr, sr, xw, wp, ys, gt, ps, pr, ow, r2s, r2, na, nb,
    kv, qd, ob, outb, send_sem, recv_sem,
):
    z, x, y, c = (lax.axis_index(n) for n in ("z", "x", "y", "c"))
    other = 1 - c

    def zat(d):
        return lax.rem(z + d + NZ, NZ)

    def xat(d):
        return lax.rem(x + d, NX)

    def yat(d):
        return lax.rem(y + d, NY)

    def cat(d):
        return other if d else c

    peers = [(z, x, yat(dy), cat(dc)) for dy in range(NY) for dc in range(NC) if dy or dc]
    row_peers = [(z, xat(dx), y, cat(dc)) for dx in range(1, NX) for dc in range(NC)]
    far = [(zat(d), x, y, c) for d in (-4, -3, -2, -1, 1, 2, 3, 4)]
    barrier = pltpu.get_barrier_semaphore()
    everyone = peers + row_peers + far
    for device in everyone:
        pl.semaphore_signal(barrier, inc=1, device_id=device, device_id_type=MESH)

    links = Links(send_sem, recv_sem)
    partner = (z, x, y, other)
    my_rows = pl.multiple_of(64 * c + 16 * y, 16)

    partial = nn(x_ref[...], sel_ref[...])
    part[...] = partial
    part16[...] = partial.astype(BF16)
    xw[z, x] = wo_ref[...]
    ids[0, :, pl.ds(pl.multiple_of(128 * x, 128), 128)] = ids_ref[...]
    pl.semaphore_wait(barrier, len(everyone))

    slot_rs = links.slots(8)
    for dy in range(NY):
        for dc in range(NC):
            if dy or dc:
                ty, tc = yat(dy), cat(dc)
                rows = pl.multiple_of(64 * tc + 16 * ty, 16)
                links.start(part16.at[pl.ds(rows, 16)], rs1.at[dy * 2 + dc], (z, x, ty, tc), slot_rs + dy * 2 + dc)

    slot_x0 = links.slots(2)
    for hh in range(2):
        links.start(wp_ref.at[hh], wp.at[z, x], (z, 2 * c + hh, y, 1 - x // 2), slot_x0 + lax.rem(x, 2))
    slot_i1 = links.slots(4)
    row_part = pl.ds(pl.multiple_of(128 * x, 128), 128)
    for dx in range(1, NX):
        links.start(ids_ref, ids.at[0, :, row_part], (z, xat(dx), y, c), slot_i1 + dx)

    slot_wo = {d: links.slots(1) for d in (-7, -6, -5, -4, -3, -2, -1, 1, 2, 3, 4, 5, 6, 7, 8)}
    slot_wp = {d: links.slots(1) for d in (-7, -6, -5, -4, -3, -2, -1, 1, 2, 3, 4, 5, 6, 7, 8)}
    ringed = pl.ds(pl.multiple_of(2 * other, 2), 2)

    def hops(phase):
        right = [2 * phase - 1, 2 * phase]
        left = [-d for d in right if d < 8]
        return right + left

    def ring_out(phase):
        for sign in (1, -1):
            block = zat(-sign * 2 * (phase - 1))
            for near in (1, 2):
                far_by = sign * (2 * (phase - 1) + near)
                if far_by != -8:
                    links.start(
                        wo_ref if phase == 1 else xw.at[block, x],
                        xw.at[block, x],
                        (zat(sign * near), x, y, c),
                        slot_wo[far_by],
                    )

    def ring_proj(phase):
        for sign in (1, -1):
            block = zat(-sign * 2 * (phase - 1))
            for near in (1, 2):
                far_by = sign * (2 * (phase - 1) + near)
                if far_by != -8:
                    links.start(
                        wp.at[block, ringed],
                        wp.at[block, ringed],
                        (zat(sign * near), x, y, c),
                        slot_wp[far_by],
                    )

    def ring_wait(phase, slots, at):
        for d in hops(phase):
            links.wait(at(zat(-d)), slots[d], (zat(1 if d > 0 else -1), x, y, c))

    def wo_at(block):
        return xw.at[block, x]

    def wp_at(block):
        return wp.at[block, ringed]

    groups = [[0, -1, 1, -2, 2], [-3, 3, -4, 4], [-5, 5, -6, 6], [-7, 7, 8]]
    slot_xw = [links.slots(4) for _ in groups]
    first_xw = [links.sends + 3 * g for g in range(len(groups))]
    links.sends += 3 * len(groups)

    def spread(g, members):
        for d in members:
            block = zat(-d)
            for dx in range(1, NX):
                links.copy(
                    xw.at[block, x], xw.at[block, x], (z, xat(dx), y, c), slot_xw[g] + dx, first_xw[g] + dx - 1
                ).start()

    ring_out(1)
    for dx in range(1, NX):
        links.wait(ids.at[0, :, row_part], slot_i1 + dx, (z, xat(dx), y, c))
    slot_i2 = links.slots(5)
    for dz in range(1, 5):
        links.start(ids.at[0], ids.at[dz], (zat(dz), x, y, c), slot_i2 + dz)

    total = part[pl.ds(my_rows, 16), :]
    for k in range(1, 8):
        links.wait(rs1.at[k], slot_rs + k, partner)
        total = total + rs1[k].astype(F32)
    sb[pl.ds(my_rows, 16), :] = total.astype(BF16)
    slot_ag = links.slots(8)
    for dy in range(NY):
        for dc in range(NC):
            if dy or dc:
                mine = sb.at[pl.ds(my_rows, 16)]
                links.start(mine, mine, (z, x, yat(dy), cat(dc)), slot_ag + dy * 2 + dc)

    for k in range(2):
        links.wait(wp.at[z, x], slot_x0 + k, partner)
    ring_wait(1, slot_wo, wo_at)
    ring_out(2)
    spread(0, groups[0][:4])
    ring_proj(1)

    for k in range(1, 8):
        links.wait(sb.at[pl.ds(my_rows, 16)], slot_ag + k, partner)
    for dz in range(1, 5):
        links.wait(ids.at[dz], slot_i2 + dz, (zat(dz), x, y, c))

    values = x_ref[...].astype(F32)
    step = softplus(nn(sb[:, :RANK], stepw_ref[...]) + bias_ref[...])
    last = [jnp.broadcast_to(ids[0, :, 128 * k + 127 : 128 * k + 128], (1, 128)) for k in range(NX)]
    prior = jnp.broadcast_to(ids[1, :, 511:512], (1, 128))
    prior = jnp.where(z == 0, jnp.full_like(prior, -1.0), prior)
    for k in range(1, NX):
        prior = jnp.where(x == k, last[k - 1], prior)
    column = jnp.transpose(jnp.broadcast_to(ids_ref[...], (128, 128)))
    before = pltpu.roll(column, 1, axis=0)
    before = jnp.where(iota((128, 128), 0) == 0, jnp.broadcast_to(prior, (128, 128)), before)
    linked = column == before
    for k in range(4):
        cols = slice(128 * k, 128 * k + 128)
        dt2[:, cols] = jnp.where(linked, step[:, cols], RESET)
    ss[x] = jnp.sum(dt2[...], axis=0, keepdims=True)
    slot_ss = links.slots(4)
    for dx in range(1, NX):
        links.start(ss.at[x], ss.at[x], (z, xat(dx), y, c), slot_ss + dx)

    driven = (step * values).astype(BF16)
    pick = (lax.rem(iota((256, 128), 0), STATE) == iota((256, 128), 1)).astype(BF16)
    inputs = nt(pick, sb[:, RANK:])

    for k in range(8):
        token = iota((256, 128), 0) // STATE + k * 16
        spread_in = jnp.where(iota((256, 128), 1) == token, inputs, 0.0).astype(BF16)
        bx[256 * k : 256 * k + 256, :] = nn(spread_in, driven)
    ring_wait(2, slot_wo, wo_at)
    ring_out(3)
    rate = a_ref[...]

    def scan(initial, keep_states):
        def advance(k, h):
            steps = dt2[pl.ds(pl.multiple_of(k * 8, 8), 8), :]
            for j in range(8):
                at = pl.ds(pl.multiple_of(k * 128 + j * 16, 16), 16)
                h = jnp.exp2(rate * steps[j : j + 1, :]) * h + bx[at, :]
                if keep_states:
                    hb[at, :] = h.astype(BF16)
            return h

        return lax.fori_loop(0, 16, advance, initial)

    hs[x] = scan(jnp.zeros((STATE, 512), F32), False).astype(BF16)
    slot_hs = links.slots(4)
    for dx in range(1, NX):
        links.start(hs.at[x], hs.at[x], (z, xat(dx), y, c), slot_hs + dx)
    spread(0, groups[0][4:])
    spread(1, groups[1])
    for dx in range(1, NX):
        links.wait(ss.at[x], slot_ss + dx, (z, xat(dx), y, c))
        links.wait(hs.at[x], slot_hs + dx, (z, xat(dx), y, c))
    running = jnp.zeros((STATE, 512), F32)
    steps_sum = jnp.zeros((1, 512), F32)
    own_prior, own_steps = running, steps_sum
    for k in range(NX):
        own_prior = jnp.where(x == k, running, own_prior)
        own_steps = jnp.where(x == k, steps_sum, own_steps)
        running = jnp.exp2(rate * ss[k]) * running + hs[k].astype(F32)
        steps_sum = steps_sum + ss[k]
    hr[...] = running.astype(BF16)
    sr[...] = steps_sum
    slot_hz, slot_sz = links.slots(5), links.slots(5)
    for dz in range(1, 5):
        links.start(hr, hz.at[dz - 1], (zat(dz), x, y, c), slot_hz + dz)
        links.start(sr, sz.at[dz - 1], (zat(dz), x, y, c), slot_sz + dz)
    ring_wait(3, slot_wo, wo_at)
    ring_out(4)
    spread(2, groups[2])
    for dz in range(1, 5):
        links.wait(hz.at[dz - 1], slot_hz + dz, (zat(dz), x, y, c))
        links.wait(sz.at[dz - 1], slot_sz + dz, (zat(dz), x, y, c))
    above = jnp.zeros((STATE, 512), F32)
    for dz in range(4, 0, -1):
        joined = jnp.exp2(rate * sz[dz - 1]) * above + hz[dz - 1].astype(F32)
        above = jnp.where(z >= dz, joined, jnp.zeros_like(joined))
    carry = jnp.exp2(rate * own_steps) * above + own_prior
    ring_wait(1, slot_wp, wp_at)
    ring_proj(2)
    scan(carry, True)
    ring_wait(4, slot_wo, wo_at)
    spread(3, groups[3])
    pick_out = (lax.rem(iota((256, 128), 0), STATE) + STATE == iota((256, 128), 1)).astype(BF16)
    own_token = iota((16, 256), 1) // STATE == iota((16, 256), 0)

    for k in range(8):
        rows = slice(16 * k, 16 * k + 16)
        coef = nt(sb[rows, RANK:], pick_out)
        coef = jnp.where(own_token, coef, 0.0).astype(BF16)
        ys[rows, :] = nn(coef, hb[256 * k : 256 * k + 256, :])
    gate = g_ref[...].astype(F32)
    mixed = (ys[...] + skip_ref[...] * values) * (gate / (1.0 + jnp.exp(-gate)))
    gt[...] = mixed.astype(BF16)

    slot_pr = [links.slots(1) for _ in groups]
    slot_r2 = [links.slots(4) for _ in groups]
    first_pr = [links.sends + g for g in range(len(groups))]
    first_r2 = [links.sends + len(groups) + 3 * g for g in range(len(groups))]
    links.sends += 4 * len(groups)
    half_rows = pl.ds(pl.multiple_of(64 * c, 64), 64)
    their_rows = pl.ds(pl.multiple_of(64 * other, 64), 64)

    def columns(d):
        return pl.ds(pl.multiple_of(128 * zat(-d), 128), 128)

    def weight_of(d):
        return xw[zat(-d)].reshape(128, 512)

    def project_pair(g):
        for d in groups[g]:
            ps[:, columns(d)] = nt(gt[their_rows, :], weight_of(d)).astype(BF16)
        for d in groups[g]:
            piece = ps.at[:, columns(d)]
            links.copy(piece, pr.at[:, columns(d)], partner, slot_pr[g], first_pr[g]).start()

    def project_own(g):
        for d in groups[g]:
            ow[:, columns(d)] = nt(gt[half_rows, :], weight_of(d))
        width = 128 * len(groups[g])
        links.copy(ps.at[:, 0:width], pr.at[:, 0:width], partner, slot_pr[g], first_pr[g]).wait_recv()
        for d in groups[g]:
            joined = ow[:, columns(d)] + pr[:, columns(d)].astype(F32)
            ow[:, columns(d)] = joined
            r2s[:, columns(d)] = joined.astype(BF16)
        for d in groups[g]:
            for dy in range(1, NY):
                ty = yat(dy)
                piece = r2s.at[pl.ds(pl.multiple_of(16 * ty, 16), 16), columns(d)]
                links.copy(
                    piece, r2.at[dy, :, columns(d)], (z, x, ty, c), slot_r2[g] + dy, first_r2[g] + dy - 1
                ).start()

    for g in range(len(groups)):
        size = len(groups[g])
        for dx in range(1, NX):
            links.copy(
                xw.at[0:size, x], xw.at[0:size, x], (z, xat(dx), y, c), slot_xw[g] + dx, first_xw[g] + dx - 1
            ).wait_recv()
        project_pair(g)
        if g == 1:
            ring_wait(2, slot_wp, wp_at)
            ring_proj(3)
        project_own(g)
    ring_wait(3, slot_wp, wp_at)
    ring_proj(4)
    stream = ow[pl.ds(pl.multiple_of(16 * y, 16), 16), :] + res_ref[pl.ds(my_rows, 16), :].astype(F32)
    for g in range(len(groups)):
        width = 128 * len(groups[g])
        for dy in range(1, NY):
            links.wait(r2.at[dy, :, 0:width], slot_r2[g] + dy, partner)
    for dy in range(1, NY):
        stream = stream + r2[dy].astype(F32)
    stream = stream.astype(BF16).astype(F32)
    normed = stream * lax.rsqrt(jnp.mean(stream * stream, axis=-1, keepdims=True) + EPS) * gain_ref[...]
    normed = normed.astype(BF16)

    na[x, y] = normed[:, :1024]
    nb[x, y] = normed[:, 1024:]
    slot_n1, slot_n2 = links.slots(4), links.slots(4)
    slot_n3 = [links.slots(4) for _ in range(4)]
    slot_n4 = [links.slots(4) for _ in range(4)]
    for d in range(1, 4):
        links.start(na.at[x, y], na.at[x, y], (z, xat(d), y, c), slot_n1 + d)
        links.start(nb.at[x, y], nb.at[x, y], (z, x, yat(d), c), slot_n2 + d)

    def over_y(k):
        piece = na.at[xat(k), y]
        for d in range(1, 4):
            links.start(piece, piece, (z, x, yat(d), c), slot_n3[k] + d)

    def over_x(k):
        piece = nb.at[x, yat(k)]
        for d in range(1, 4):
            links.start(piece, piece, (z, xat(d), y, c), slot_n4[k] + d)

    over_y(0)
    over_x(0)
    for k in (3, 1, 2):
        links.wait(na.at[x, y], slot_n1 + 4 - k, partner)
        over_y(k)
        links.wait(nb.at[x, y], slot_n2 + 4 - k, partner)
        over_x(k)
    ring_wait(4, slot_wp, wp_at)
    slot_pw = links.slots(1)
    links.start(wp.at[:, ringed], wp.at[:, ringed], partner, slot_pw)
    for k in range(NX):
        qd[k] = jnp.transpose(jnp.broadcast_to(ids[0, :, 128 * k : 128 * k + 128], (128, 128)))
    q_doc = jnp.concatenate([qd[k, half_rows, :] for k in range(NX)], axis=0)
    q_doc = jnp.concatenate([q_doc] * 4, axis=1)
    row_of = iota((256, 512), 0)
    in_row = 128 * (row_of // 64) + 64 * c + lax.rem(row_of, 64)

    links.wait(wp.at[:, ringed], slot_pw, partner)
    for k in range(4):
        for d in range(1, 4):
            links.wait(na.at[x, y], slot_n3[k] + d, partner)
            links.wait(nb.at[x, y], slot_n4[k] + d, partner)
    triple = nn(na[...].reshape(256, 1024), wp[0:8].reshape(1024, 384))
    triple = triple + nn(nb[...].reshape(256, 1024), wp[8:16].reshape(1024, 384))
    query = triple[:, :HEAD].astype(BF16)
    kv[0, :, c] = triple[:, HEAD:].astype(BF16).reshape(4, 64, 256)

    slot_kz = [links.slots(4) for _ in range(5)]
    slot_kc = [links.slots(4) for _ in range(5)]

    def chunk(d, part_of, core):
        return kv.at[d, part_of, core]

    def pass_on(d, part_of):
        if d < 4:
            links.start(chunk(d, part_of, c), chunk(d + 1, part_of, c), (zat(1), x, y, c), slot_kz[d + 1] + part_of)
        links.start(chunk(d, part_of, c), chunk(d, part_of, c), partner, slot_kc[d] + part_of)

    top = jnp.full((256, 1), HIDDEN, F32)
    mass = jnp.zeros((256, 1), F32)
    acc = jnp.zeros((256, HEAD), F32)

    def attend(d, carried):
        top, mass, acc = carried
        for p in range(4):
            links.wait(chunk(d, p, other), slot_kc[d] + p, partner)
        block = kv[d].reshape(512, 256)
        scores = nt(query, block[:, :HEAD]) * (HEAD**-0.5 * LOG2E)
        k_doc = jnp.where(z >= d, ids[d], -1.0)
        allowed = jnp.broadcast_to(k_doc, (256, 512)) == q_doc
        ahead = iota((256, 512), 1) - in_row
        if d == 0:
            allowed = allowed & (ahead <= 0)
        if d == 4:
            allowed = allowed & (ahead > 0)
        scores = jnp.where(allowed, scores, HIDDEN)
        new_top = jnp.maximum(top, jnp.max(scores, axis=-1, keepdims=True))
        probs = jnp.exp2(scores - new_top)
        shrink = jnp.exp2(top - new_top)
        mass = mass * shrink + jnp.sum(probs, axis=-1, keepdims=True)
        acc = acc * shrink + nn(probs.astype(BF16), block[:, HEAD:])
        return new_top, mass, acc

    carried = (top, mass, acc)
    for p in range(4):
        pass_on(0, p)
    for d in range(1, 5):
        for p in range(4):
            links.wait(chunk(d, p, c), slot_kz[d] + p, partner)
            pass_on(d, p)
        carried = attend(d - 1, carried)
    top, mass, acc = attend(4, carried)
    ob[...] = (acc / mass).astype(BF16).reshape(4, 64, HEAD)

    slot_o = links.slots(4)
    mine = slot_o + lax.rem(x, 2) * 2 + c
    cols = pl.ds(pl.multiple_of(128 * lax.rem(x, 2), 128), 128)
    for dx in range(1, NX):
        tx = xat(dx)
        links.start(ob.at[tx], outb.at[half_rows, cols], (z, tx, y, x // 2), mine)
    stays = c == x // 2
    to_partner = links.copy(ob.at[x], outb.at[half_rows, cols], partner, mine)

    @pl.when(stays)
    def _():
        outb[half_rows, cols] = ob[x]

    @pl.when(jnp.logical_not(stays))
    def _():
        to_partner.start()

    for k in range(4):
        from_me = stays & (lax.rem(x, 2) * 2 + c == k)

        @pl.when(jnp.logical_not(from_me))
        def _():
            links.wait(outb.at[half_rows, cols], slot_o + k, partner)

    out_ref[...] = outb[...]

    @pl.when(jnp.logical_not(stays))
    def _():
        to_partner.wait_send()

    links.drain()
    for g in range(len(groups)):
        size, width = len(groups[g]), 128 * len(groups[g])
        for d in range(1, 4):
            links.copy(xw.at[0:size, x], xw.at[0:size, x], partner, slot_xw[g] + d, first_xw[g] + d - 1).wait_send()
            rows = r2.at[d, :, 0:width]
            links.copy(rows, rows, partner, slot_r2[g] + d, first_r2[g] + d - 1).wait_send()
        links.copy(ps.at[:, 0:width], pr.at[:, 0:width], partner, slot_pr[g], first_pr[g]).wait_send()
    assert links.sends <= SENDS and links.recvs <= RECVS, (links.sends, links.recvs)


SENDS, RECVS = 224, 240


def body(
    mixer_input, gate_input, document_ids, residual, select_weight, step_weight, step_bias, decay_log, skip_gain,
    out_weight, norm_gain, project_weight,
):
    vmem = pl.BlockSpec(memory_space=pltpu.VMEM)
    operands = (
        mixer_input,
        gate_input,
        document_ids.astype(F32).reshape(1, 128),
        residual,
        jnp.pad(select_weight, ((0, 0), (0, 96))),
        step_weight,
        step_bias.reshape(1, 512),
        -jnp.exp(decay_log).T * LOG2E,
        skip_gain.reshape(1, 512),
        out_weight.T,
        norm_gain.reshape(1, 2048),
        project_weight.reshape(32, 3, 2, 128).transpose(2, 0, 1, 3).reshape(2, 32, 384),
    )
    scratch = [
        pltpu.VMEM((128, 256), F32),
        pltpu.VMEM((128, 256), BF16),
        pltpu.VMEM((8, 16, 256), BF16),
        pltpu.VMEM((128, 256), BF16),
        pltpu.VMEM((5, 1, 512), F32),
        pltpu.VMEM((128, 512), F32),
        pltpu.VMEM((2048, 512), F32),
        pltpu.VMEM((2048, 512), BF16),
        pltpu.VMEM((4, 16, 512), BF16),
        pltpu.VMEM((4, 1, 512), F32),
        pltpu.VMEM((4, 16, 512), BF16),
        pltpu.VMEM((4, 1, 512), F32),
        pltpu.VMEM((16, 512), BF16),
        pltpu.VMEM((1, 512), F32),
        pltpu.VMEM((16, 4, 32, 512), BF16),
        pltpu.VMEM((16, 4, 32, 384), BF16),
        pltpu.VMEM((128, 512), F32),
        pltpu.VMEM((128, 512), BF16),
        pltpu.VMEM((64, 2048), BF16),
        pltpu.VMEM((64, 2048), BF16),
        pltpu.VMEM((64, 2048), F32),
        pltpu.VMEM((64, 2048), BF16),
        pltpu.VMEM((4, 16, 2048), BF16),
        pltpu.VMEM((4, 4, 16, 1024), BF16),
        pltpu.VMEM((4, 4, 16, 1024), BF16),
        pltpu.VMEM((5, 4, 2, 64, 256), BF16),
        pltpu.VMEM((4, 128, 128), F32),
        pltpu.VMEM((4, 64, 128), BF16),
        pltpu.VMEM((128, 256), BF16),
        pltpu.SemaphoreType.DMA((SENDS,)),
        pltpu.SemaphoreType.DMA((RECVS,)),
    ]
    return pl.pallas_call(
        kernel,
        out_shape=jax.ShapeDtypeStruct((128, 256), BF16),
        in_specs=[vmem] * len(operands),
        out_specs=vmem,
        scratch_shapes=scratch,
        compiler_params=pltpu.CompilerParams(collective_id=0, has_side_effects=True, vmem_limit_bytes=48 << 20),
    )(*operands)


def solution(mesh):
    split = Mesh(mesh.devices.reshape(NZ, NX, NY, NC), ("z", "x", "y", "c"))
    placed = (
        P(SEQ, TP), P(SEQ, TP), P(SEQ), P(SEQ, None), P(TP, None), P(None, TP), P(TP), P(TP, None), P(TP),
        P(TP, SEQ), P(), P(SEQ, None, TP),
    )
    return jax.shard_map(body, mesh=split, in_specs=placed, out_specs=P(SEQ, TP), check_vma=False)
```

```python
import math

import jax
import jax.numpy as jnp
from jax import lax
from jax.experimental import pallas as pl
from jax.experimental.pallas import tpu as pltpu
from jax.sharding import Mesh
from jax.sharding import PartitionSpec as P

MESH = pl.DeviceIdType.MESH
NZ, NX, NY, NC = 16, 4, 4, 2
STATE = 16
RANK = 128
HEAD = 128
WINDOW = 2048
EPS = 1e-05
LOG2E = 1.4426950408889634
RESET = 1e6
HIDDEN = -1e30
SEQ = ("z", "x")
TP = ("y", "c")
F32 = jnp.float32
BF16 = jnp.bfloat16


def nt(a, b):
    return lax.dot_general(a, b, (((1,), (1,)), ((), ())), preferred_element_type=F32)


def nn(a, b):
    return jnp.dot(a, b, preferred_element_type=F32)


def iota(shape, dim):
    return lax.broadcasted_iota(jnp.int32, shape, dim)


def softplus(v):
    e = jnp.exp(-jnp.abs(v))
    small = e * (1.0 - e * (0.5 - e * (1.0 / 3.0 - e * 0.25)))
    return jnp.maximum(v, 0.0) + jnp.where(e < 0.01, small, jnp.log(1.0 + e))


class Links:
    def __init__(self, send, recv):
        self.send, self.recv = send, recv
        self.recvs = 0
        self.sent = [0] * SENDS

    def slots(self, count):
        first = self.recvs
        self.recvs += count
        return first

    def copy(self, src, dst, device, slot, send):
        return pltpu.make_async_remote_copy(
            src_ref=src,
            dst_ref=dst,
            send_sem=self.send.at[send],
            recv_sem=self.recv.at[slot],
            device_id=device,
            device_id_type=MESH,
        )

    def start(self, src, dst, device, slot, send=None):
        size = math.prod(src.shape) * jnp.dtype(src.dtype).itemsize
        if send is None:
            send = 0 if self.sent[0] + size <= SEND_MOST else 1
        self.sent[send] += size
        self.copy(src, dst, device, slot, send).start()

    def wait(self, dst, slot, device):
        self.copy(dst, dst, device, slot, 0).wait_recv()

    def drain(self, send, whole, device):
        self.copy(whole, whole, device, 0, send).wait_send()


def kernel(
    *refs
):
    homes, refs = refs[:12], refs[12:]
    out_ref, refs = refs[0], refs[1:]
    staged, refs = refs[:12], refs[12:]
    x_ref, g_ref, doc_ref, res_ref, sel_ref, stepw_ref, bias_ref, a_ref, skip_ref, wo_ref, gain_ref, proj_ref = staged
    (
        part, part2, parts, ids_ref, wp_ref, ids, dt2, bx, hb, hs, ss, hz, sz, hr, sr, xw, wp, ys, gt, ps, pr, ow, r2s, r2, na, nb,
        kv, qd, ob, outb, local_sem, send_sem, recv_sem,
    ) = refs
    z, x, y, c = (lax.axis_index(n) for n in ("z", "x", "y", "c"))
    other = 1 - c

    def zat(d):
        return lax.rem(z + d + NZ, NZ)

    def xat(d):
        return lax.rem(x + d + NX, NX)

    def yat(d):
        return lax.rem(y + d, NY)

    def cat(d):
        return other if d else c

    peers = [(z, x, yat(dy), cat(dc)) for dy in range(NY) for dc in range(NC) if dy or dc]
    row_peers = [(z, xat(dx), y, cat(dc)) for dx in range(1, NX) for dc in range(NC)]
    far = [(zat(d), x, y, c) for d in (-4, -3, -2, -1, 1, 2, 3, 4)]
    barrier = pltpu.get_barrier_semaphore()
    everyone = peers + row_peers + far
    for device in everyone:
        pl.semaphore_signal(barrier, inc=1, device_id=device, device_id_type=MESH)

    links = Links(send_sem, recv_sem)
    loads = [pltpu.make_async_copy(src, dst, local_sem.at[n]) for n, (src, dst) in enumerate(zip(homes, staged))]
    early = (0, 4, 2, 9, 11)
    late = (5, 6, 7, 8, 1, 3, 10)
    for n in early + late:
        loads[n].start()
    partner = (z, x, y, other)
    my_rows = pl.multiple_of(64 * c + 16 * y, 16)

    for n in early:
        loads[n].wait()
    ids_ref[...] = doc_ref[...].astype(F32)
    for hh in range(2):
        for j in range(3):
            wp_ref[hh, :, HEAD * j : HEAD * j + HEAD] = proj_ref[j, :, HEAD * hh : HEAD * hh + HEAD]
    part[0:128] = nt(x_ref[...], sel_ref[0:RANK]).astype(BF16)
    part[128:160] = nt(sel_ref[RANK:], x_ref[...]).astype(BF16)
    xw[z, x] = wo_ref[...]
    ids[0, :, pl.ds(pl.multiple_of(128 * x, 128), 128)] = ids_ref[...]
    pl.semaphore_wait(barrier, len(everyone))

    slot_pair, slot_rs = links.slots(1), links.slots(1)
    links.start(part, parts.at[0], partner, slot_pair)

    slot_i1 = links.slots(1)
    row_part = pl.ds(pl.multiple_of(128 * x, 128), 128)
    for dx in range(1, NX):
        links.start(ids_ref, ids.at[0, :, row_part], (z, xat(dx), y, c), slot_i1, 2)
    slot_x0 = links.slots(1)
    for hh in range(2):
        links.start(wp_ref.at[hh], wp.at[z, x], (z, 2 * c + hh, y, 1 - x // 2), slot_x0)

    slot_wo, slot_wp = links.slots(4), links.slots(4)
    ringed = pl.ds(pl.multiple_of(2 * other, 2), 2)

    def ring_out(phase):
        for sign in (1, -1):
            block = zat(-sign * 2 * (phase - 1))
            for near in (1, 2):
                far_by = sign * (2 * (phase - 1) + near)
                if far_by != -8:
                    links.start(
                        wo_ref if phase == 1 else xw.at[block, x],
                        xw.at[block, x],
                        (zat(sign * near), x, y, c),
                        slot_wo + phase - 1,
                    )

    def ring_proj(phase):
        for sign in (1, -1):
            block = zat(-sign * 2 * (phase - 1))
            for near in (1, 2):
                far_by = sign * (2 * (phase - 1) + near)
                if far_by != -8:
                    links.start(
                        wp.at[block, ringed],
                        wp.at[block, ringed],
                        (zat(sign * near), x, y, c),
                        slot_wp + phase - 1,
                    )

    def ring_wait(phase):
        links.wait(xw.at[0 : 4 - phase // 4, x], slot_wo + phase - 1, partner)

    def ring_proj_wait(phase):
        links.wait(wp.at[0 : 4 - phase // 4, ringed], slot_wp + phase - 1, partner)

    groups = [[0, -1, 1, -2, 2], [-3, 3, -4, 4], [-5, 5, -6, 6], [-7, 7, 8]]
    slot_near, slot_last = [links.slots(1) for _ in groups], [links.slots(1) for _ in range(2)]

    def spread(g, members):
        for d in members:
            piece = xw.at[zat(-d), x]
            for dx in (1, 3) if g < 2 else (2, 1, 3):
                links.start(piece, piece, (z, xat(dx), y, c), slot_near[g])

    def relay(g):
        links.wait(xw.at[0 : 2 * len(groups[g]), x], slot_near[g], partner)
        middle = (len(groups[g]) + 1) // 2
        for n, d in enumerate(groups[g]):
            toward = 1 if n < middle else -1
            piece = xw.at[zat(-d), xat(-toward)]
            links.start(piece, piece, (z, xat(toward), y, c), slot_last[g])

    def arrived(g):
        if g < 2:
            links.wait(xw.at[0 : len(groups[g]), x], slot_last[g], partner)
        else:
            links.wait(xw.at[0 : 3 * len(groups[g]), x], slot_near[g], partner)

    ring_out(1)
    spread(0, groups[0][:1])
    links.wait(parts.at[0], slot_pair, partner)
    selected = part[...].astype(F32) + parts[0].astype(F32)
    part2[...] = selected.astype(BF16)
    for dy in range(1, NY):
        links.start(part2, parts.at[dy], (z, x, yat(dy), c), slot_rs)
    for n in late:
        loads[n].wait()
    links.wait(ids.at[0, :, 0:384], slot_i1, partner)
    slot_i2 = links.slots(2)
    for dz in range(1, 5):
        links.start(ids.at[0], ids.at[dz], (zat(dz), x, y, c), slot_i2 + min(dz - 1, 1), 6)

    links.wait(wp.at[z, 0:2], slot_x0, partner)
    ring_wait(1)
    ring_out(2)
    spread(0, groups[0][1:])
    ring_proj(1)
    links.wait(parts.at[1:4], slot_rs, partner)
    for k in range(1, NY):
        selected = selected + parts[k].astype(F32)
    values = x_ref[...].astype(F32)
    step = softplus(nn(selected[:RANK].astype(BF16), stepw_ref[...]) + bias_ref[...])
    column = jnp.transpose(jnp.broadcast_to(ids_ref[...], (128, 128)))
    before = pltpu.roll(column, 1, axis=0)
    linked = (column == before) | (iota((128, 128), 0) == 0)
    for k in range(4):
        cols = slice(128 * k, 128 * k + 128)
        dt2[:, cols] = jnp.where(linked, step[:, cols], RESET)
    ss[x] = jnp.sum(dt2[...], axis=0, keepdims=True)
    slot_ss = links.slots(1)
    for dx in range(1, NX):
        links.start(ss.at[x], ss.at[x], (z, xat(dx), y, c), slot_ss, 4)

    driven = (step * values).astype(BF16)
    inputs = jnp.concatenate([selected[RANK : RANK + STATE]] * 16, axis=0)
    for k in range(8):
        token = iota((256, 128), 0) // STATE + k * 16
        spread_in = jnp.where(iota((256, 128), 1) == token, inputs, 0.0).astype(BF16)
        bx[256 * k : 256 * k + 256, :] = nn(spread_in, driven)
    rate = -jnp.exp(a_ref[...]) * LOG2E

    def scan(initial, keep_states):
        def advance(k, h):
            steps = dt2[pl.ds(pl.multiple_of(k * 8, 8), 8), :]
            for j in range(8):
                at = pl.ds(pl.multiple_of(k * 128 + j * 16, 16), 16)
                h = jnp.exp2(rate * steps[j : j + 1, :]) * h + bx[at, :]
                if keep_states:
                    hb[at, :] = h.astype(BF16)
            return h

        return lax.fori_loop(0, 16, advance, initial)

    hs[x] = scan(jnp.zeros((STATE, 512), F32), False).astype(BF16)
    slot_hs = links.slots(1)
    for dx in range(1, NX):
        links.start(hs.at[x], hs.at[x], (z, xat(dx), y, c), slot_hs)
    ring_wait(2)
    ring_out(3)
    spread(1, groups[1])
    relay(0)
    links.wait(ss.at[0:3], slot_ss, partner)
    links.wait(hs.at[0:3], slot_hs, partner)
    links.wait(ids.at[1], slot_i2, partner)
    prior = jnp.where(z == 0, -1.0, ids[1, :, 511:512])
    breaks = []
    for k in range(NX):
        if k:
            prior = ids[0, :, 128 * k - 1 : 128 * k]
        first = ids[0, :, 128 * k : 128 * k + 1]
        breaks.append(jnp.broadcast_to(jnp.where(first == prior, 0.0, RESET), (1, 512)))
    running = jnp.zeros((STATE, 512), F32)
    steps_sum = jnp.zeros((1, 512), F32)
    own_prior, own_steps, own_break = running, steps_sum, steps_sum
    for k in range(NX):
        own_prior = jnp.where(x == k, running, own_prior)
        own_steps = jnp.where(x == k, steps_sum, own_steps)
        own_break = jnp.where(x == k, breaks[k], own_break)
        steps_of = ss[k] + breaks[k]
        running = jnp.exp2(rate * steps_of) * running + hs[k].astype(F32)
        steps_sum = steps_sum + steps_of
    dt2[0:1, :] = dt2[0:1, :] + own_break
    hr[...] = running.astype(BF16)
    sr[...] = steps_sum
    slot_hz, slot_sz = links.slots(1), links.slots(1)
    for dz in range(1, 5):
        links.start(hr, hz.at[dz - 1], (zat(dz), x, y, c), slot_hz)
        links.start(sr, sz.at[dz - 1], (zat(dz), x, y, c), slot_sz, 5)
    ring_wait(3)
    ring_out(4)
    spread(2, groups[2])
    relay(1)
    links.wait(hz, slot_hz, partner)
    links.wait(sz, slot_sz, partner)
    above = jnp.zeros((STATE, 512), F32)
    for dz in range(4, 0, -1):
        joined = jnp.exp2(rate * sz[dz - 1]) * above + hz[dz - 1].astype(F32)
        above = jnp.where(z >= dz, joined, jnp.zeros_like(joined))
    carry = jnp.exp2(rate * own_steps) * above + own_prior
    ring_proj_wait(1)
    ring_proj(2)
    scan(carry, True)
    ring_wait(4)
    spread(3, groups[3])
    pick_out = (lax.rem(iota((STATE, 256), 1), STATE) == iota((STATE, 256), 0)).astype(BF16)
    coefs = lax.dot_general(
        selected[RANK + STATE :].astype(BF16), pick_out, (((0,), (0,)), ((), ())), preferred_element_type=F32
    )
    own_token = iota((16, 256), 1) // STATE == iota((16, 256), 0)

    for k in range(8):
        rows = slice(16 * k, 16 * k + 16)
        coef = jnp.where(own_token, coefs[rows], 0.0).astype(BF16)
        ys[rows, :] = nn(coef, hb[256 * k : 256 * k + 256, :])
    gate = g_ref[...].astype(F32)
    mixed = (ys[...] + skip_ref[...] * values) * (gate / (1.0 + jnp.exp(-gate)))
    gt[...] = mixed.astype(BF16)

    slot_pr = [links.slots(1) for _ in groups]
    slot_r2 = [links.slots(1) for _ in groups]
    half_rows = pl.ds(pl.multiple_of(64 * c, 64), 64)
    their_rows = pl.ds(pl.multiple_of(64 * other, 64), 64)

    def columns(d):
        return pl.ds(pl.multiple_of(128 * zat(-d), 128), 128)

    def weight_of(d):
        return xw[zat(-d)].reshape(128, 512)

    def project_pair(g):
        for d in groups[g]:
            ps[:, columns(d)] = nt(gt[their_rows, :], weight_of(d)).astype(BF16)
        for d in groups[g]:
            piece = ps.at[:, columns(d)]
            links.start(piece, pr.at[:, columns(d)], partner, slot_pr[g])

    def project_own(g):
        for d in groups[g]:
            ow[:, columns(d)] = nt(gt[half_rows, :], weight_of(d))
        width = 128 * len(groups[g])
        links.wait(pr.at[:, 0:width], slot_pr[g], partner)
        for d in groups[g]:
            joined = ow[:, columns(d)] + pr[:, columns(d)].astype(F32)
            ow[:, columns(d)] = joined
            r2s[:, columns(d)] = joined.astype(BF16)
        for d in groups[g]:
            for dy in range(1, NY):
                ty = yat(dy)
                piece = r2s.at[pl.ds(pl.multiple_of(16 * ty, 16), 16), columns(d)]
                links.start(piece, r2.at[dy, :, columns(d)], (z, x, ty, c), slot_r2[g], 1)

    arrived(0)
    project_pair(0)
    arrived(1)
    project_pair(1)
    project_own(0)
    project_own(1)
    ring_proj_wait(2)
    ring_proj(3)
    arrived(2)
    project_pair(2)
    project_own(2)
    arrived(3)
    project_pair(3)
    project_own(3)
    stream = ow[pl.ds(pl.multiple_of(16 * y, 16), 16), :] + res_ref[pl.ds(my_rows, 16), :].astype(F32)
    for g in range(len(groups)):
        width = 128 * len(groups[g])
        links.wait(r2.at[0:3, :, 0:width], slot_r2[g], partner)
    for dy in range(1, NY):
        stream = stream + r2[dy].astype(F32)
    links.wait(ids.at[2:5], slot_i2 + 1, partner)
    stream = stream.astype(BF16).astype(F32)
    normed = stream * lax.rsqrt(jnp.mean(stream * stream, axis=-1, keepdims=True) + EPS) * gain_ref[...]
    normed = normed.astype(BF16)

    na[x, y] = normed[:, :1024]
    nb[x, y] = normed[:, 1024:]
    slot_n1, slot_n2 = links.slots(3), links.slots(3)
    slot_n3, slot_n4 = links.slots(1), links.slots(1)
    for d in range(1, 4):
        links.start(na.at[x, y], na.at[x, y], (z, xat(d), y, c), slot_n1 + d - 1)
        links.start(nb.at[x, y], nb.at[x, y], (z, x, yat(d), c), slot_n2 + d - 1)

    def over_y(k):
        piece = na.at[xat(k), y]
        for d in range(1, 4):
            links.start(piece, piece, (z, x, yat(d), c), slot_n3)

    def over_x(k):
        piece = nb.at[x, yat(k)]
        for d in range(1, 4):
            links.start(piece, piece, (z, xat(d), y, c), slot_n4)

    over_y(0)
    over_x(0)
    ring_proj_wait(3)
    ring_proj(4)

    for k in range(NX):
        qd[k] = jnp.transpose(jnp.broadcast_to(ids[0, :, 128 * k : 128 * k + 128], (128, 128)))
    q_doc = jnp.concatenate([qd[k, half_rows, :] for k in range(NX)], axis=0)
    row_of = iota((256, 128), 0)
    in_row = 128 * (row_of // 64) + 64 * c + lax.rem(row_of, 64)
    for k in (3, 1, 2):
        links.wait(na.at[x, y], slot_n1 + 3 - k, partner)
        over_y(k)
        links.wait(nb.at[x, y], slot_n2 + 3 - k, partner)
        over_x(k)
    ring_proj_wait(4)
    slot_pw = links.slots(1)
    links.start(wp.at[:, ringed], wp.at[:, ringed], partner, slot_pw)

    slot_kz = [None] + [links.slots(4) for _ in range(4)]
    slot_kc = links.slots(5)

    def chunk(d, k, core):
        return kv.at[d, xat(k), core]

    def pass_on(d, k):
        if d < 4:
            links.start(chunk(d, k, c), chunk(d + 1, k, c), (zat(1), x, y, c), slot_kz[d + 1] + k)
        links.start(chunk(d, k, c), chunk(d, k, c), partner, slot_kc + d)

    def forward(d, k):
        links.wait(chunk(d, k, c), slot_kz[d] + k, partner)
        pass_on(d, k)

    links.wait(na.at[0:3], slot_n3, partner)
    links.wait(nb.at[0:3], slot_n4, partner)
    links.wait(wp.at[:, ringed], slot_pw, partner)
    made = nn(na[...].reshape(256, 1024), wp[0:8].reshape(1024, 384))
    made = made + nn(nb[...].reshape(256, 1024), wp[8:16].reshape(1024, 384))
    query = made[:, :HEAD].astype(BF16)
    kv[0, :, c] = made[:, HEAD:].astype(BF16).reshape(4, 64, 256)
    for k in range(4):
        pass_on(0, k)

    def attend(d, carried, blocks):
        top, mass, acc = carried
        links.wait(kv.at[d, :, other], slot_kc + d, partner)
        scores, places = [], []
        for k in blocks:
            place = xat(k)
            piece = nt(query, kv[d, place, :, :, :HEAD].reshape(128, HEAD)) * (HEAD**-0.5 * LOG2E)
            k_doc = jnp.where(z >= d, ids[d, :, pl.ds(pl.multiple_of(128 * place, 128), 128)], -1.0)
            allowed = jnp.broadcast_to(k_doc, (256, 128)) == q_doc
            ahead = iota((256, 128), 1) + 128 * place - in_row
            if d == 0:
                allowed = allowed & (ahead <= 0)
            if d == 4:
                allowed = allowed & (ahead > 0)
            scores.append(jnp.where(allowed, piece, HIDDEN))
            places.append(place)
        highest = scores[0]
        for piece in scores[1:]:
            highest = jnp.maximum(highest, piece)
        new_top = jnp.maximum(top, jnp.max(highest, axis=-1, keepdims=True))
        shrink = jnp.exp2(top - new_top)
        acc = acc * shrink
        added = jnp.zeros((256, 128), F32)
        for place, piece in zip(places, scores):
            probs = jnp.exp2(piece - new_top)
            added = added + probs
            acc = acc + nn(probs.astype(BF16), kv[d, place, :, :, HEAD:].reshape(128, HEAD))
        mass = mass * shrink + jnp.sum(added, axis=-1, keepdims=True)
        return new_top, mass, acc

    carried = (jnp.full((256, 1), HIDDEN, F32), jnp.zeros((256, 1), F32), jnp.zeros((256, HEAD), F32))
    every = (0, 1, 2, 3)
    for d in range(1, 4):
        for k in range(4):
            forward(d, k)
        carried = attend(d - 1, carried, every)
    for k in range(4):
        forward(4, k)
    carried = attend(3, carried, every)
    top, mass, acc = attend(4, carried, every)
    ob[...] = (acc / mass).astype(BF16).reshape(4, 64, HEAD)

    slot_o = links.slots(4)
    mine = slot_o + lax.rem(x, 2) * 2 + c
    cols = pl.ds(pl.multiple_of(128 * lax.rem(x, 2), 128), 128)
    for dx in range(1, NX):
        tx = xat(dx)
        links.start(ob.at[tx], outb.at[half_rows, cols], (z, tx, y, x // 2), mine)
    stays = c == x // 2
    to_partner = links.copy(ob.at[x], outb.at[half_rows, cols], partner, mine, 3)

    @pl.when(stays)
    def _():
        outb[half_rows, cols] = ob[x]

    @pl.when(jnp.logical_not(stays))
    def _():
        to_partner.start()

    for k in range(4):
        from_me = stays & (lax.rem(x, 2) * 2 + c == k)

        @pl.when(jnp.logical_not(from_me))
        def _():
            links.wait(outb.at[half_rows, cols], slot_o + k, partner)

    out_ref[...] = outb[...]

    @pl.when(jnp.logical_not(stays))
    def _():
        to_partner.wait_send()

    for send in range(2):
        assert links.sent[send] % 16384 == 0
        links.drain(send, bx.at[0 : links.sent[send] // 2048], partner)
    links.drain(2, ids.at[0, :, 0:384], partner)
    links.drain(4, ss.at[0:3], partner)
    links.drain(5, sz, partner)
    links.drain(6, ids.at[0:4], partner)
    assert links.recvs <= RECVS, links.recvs


SENDS, RECVS = 7, 68
SEND_MOST = 4 << 20


def body(
    mixer_input, gate_input, document_ids, residual, select_weight, step_weight, step_bias, decay_log, skip_gain,
    out_weight, norm_gain, project_weight,
):
    vmem = pl.BlockSpec(memory_space=pltpu.VMEM)
    hbm = pl.BlockSpec(memory_space=pltpu.HBM)
    operands = (
        mixer_input,
        gate_input,
        document_ids.reshape(1, 128),
        residual,
        select_weight.T,
        step_weight,
        step_bias.reshape(1, 512),
        decay_log.T,
        skip_gain.reshape(1, 512),
        out_weight.T,
        norm_gain.reshape(1, 2048),
        project_weight.transpose(1, 0, 2),
    )
    scratch = [pltpu.VMEM(o.shape, o.dtype) for o in operands]
    scratch += [
        pltpu.VMEM((160, 128), BF16),
        pltpu.VMEM((160, 128), BF16),
        pltpu.VMEM((4, 160, 128), BF16),
        pltpu.VMEM((1, 128), F32),
        pltpu.VMEM((2, 32, 384), BF16),
        pltpu.VMEM((5, 1, 512), F32),
        pltpu.VMEM((128, 512), F32),
        pltpu.VMEM((2048, 512), F32),
        pltpu.VMEM((2048, 512), BF16),
        pltpu.VMEM((4, 16, 512), BF16),
        pltpu.VMEM((4, 1, 512), F32),
        pltpu.VMEM((4, 16, 512), BF16),
        pltpu.VMEM((4, 1, 512), F32),
        pltpu.VMEM((16, 512), BF16),
        pltpu.VMEM((1, 512), F32),
        pltpu.VMEM((16, 4, 32, 512), BF16),
        pltpu.VMEM((16, 4, 32, 384), BF16),
        pltpu.VMEM((128, 512), F32),
        pltpu.VMEM((128, 512), BF16),
        pltpu.VMEM((64, 2048), BF16),
        pltpu.VMEM((64, 2048), BF16),
        pltpu.VMEM((64, 2048), F32),
        pltpu.VMEM((64, 2048), BF16),
        pltpu.VMEM((4, 16, 2048), BF16),
        pltpu.VMEM((4, 4, 16, 1024), BF16),
        pltpu.VMEM((4, 4, 16, 1024), BF16),
        pltpu.VMEM((5, 4, 2, 64, 256), BF16),
        pltpu.VMEM((4, 128, 128), F32),
        pltpu.VMEM((4, 64, 128), BF16),
        pltpu.VMEM((128, 256), BF16),
        pltpu.SemaphoreType.DMA((12,)),
        pltpu.SemaphoreType.DMA((SENDS,)),
        pltpu.SemaphoreType.DMA((RECVS,)),
    ]
    return pl.pallas_call(
        kernel,
        out_shape=jax.ShapeDtypeStruct((128, 256), BF16),
        in_specs=[hbm] * len(operands),
        out_specs=vmem,
        scratch_shapes=scratch,
        compiler_params=pltpu.CompilerParams(collective_id=0, has_side_effects=True, vmem_limit_bytes=67043328),
    )(*operands)


def solution(mesh):
    split = Mesh(mesh.devices.reshape(NZ, NX, NY, NC), ("z", "x", "y", "c"))
    placed = (
        P(SEQ, TP), P(SEQ, TP), P(SEQ), P(SEQ, None), P(TP, None), P(None, TP), P(TP), P(TP, None), P(TP),
        P(TP, SEQ), P(), P(SEQ, None, TP),
    )
    return jax.shard_map(body, mesh=split, in_specs=placed, out_specs=P(SEQ, TP), check_vma=False)
```

```python
import math

import jax
import jax.numpy as jnp
from jax import lax
from jax.experimental import pallas as pl
from jax.experimental.pallas import tpu as pltpu
from jax.sharding import Mesh
from jax.sharding import PartitionSpec as P

MESH = pl.DeviceIdType.MESH
NZ, NX, NY, NC = 16, 4, 4, 2
STATE = 16
RANK = 128
HEAD = 128
WINDOW = 2048
EPS = 1e-05
LOG2E = 1.4426950408889634
RESET = 1e6
HIDDEN = -1e30
SEQ = ("z", "x")
TP = ("y", "c")
F32 = jnp.float32
BF16 = jnp.bfloat16


def nt(a, b):
    return lax.dot_general(a, b, (((1,), (1,)), ((), ())), preferred_element_type=F32)


def nn(a, b):
    return jnp.dot(a, b, preferred_element_type=F32)


def iota(shape, dim):
    return lax.broadcasted_iota(jnp.int32, shape, dim)


def softplus(v):
    e = jnp.exp(-jnp.abs(v))
    small = e * (1.0 - e * (0.5 - e * (1.0 / 3.0 - e * 0.25)))
    return jnp.maximum(v, 0.0) + jnp.where(e < 0.01, small, jnp.log(1.0 + e))


class Links:
    def __init__(self, send, recv):
        self.send, self.recv = send, recv
        self.recvs = 0
        self.sent = [0] * SENDS

    def slots(self, count):
        first = self.recvs
        self.recvs += count
        return first

    def copy(self, src, dst, device, slot, send):
        return pltpu.make_async_remote_copy(
            src_ref=src,
            dst_ref=dst,
            send_sem=self.send.at[send],
            recv_sem=self.recv.at[slot],
            device_id=device,
            device_id_type=MESH,
        )

    def start(self, src, dst, device, slot, send=None):
        size = math.prod(src.shape) * jnp.dtype(src.dtype).itemsize
        if send is None:
            send = 0 if self.sent[0] + size <= SEND_MOST else 1
        self.sent[send] += size
        self.copy(src, dst, device, slot, send).start()

    def wait(self, dst, slot, device):
        self.copy(dst, dst, device, slot, 0).wait_recv()

    def drain(self, send, whole, device):
        self.copy(whole, whole, device, 0, send).wait_send()


def kernel(
    *refs
):
    homes, refs = refs[:12], refs[12:]
    out_ref, refs = refs[0], refs[1:]
    staged, refs = refs[:12], refs[12:]
    x_ref, g_ref, doc_ref, res_ref, sel_ref, stepw_ref, bias_ref, a_ref, skip_ref, wo_ref, gain_ref, proj_ref = staged
    (
        part, part2, parts, ids_ref, wp_ref, ids, dt2, bx, hb, hs, ss, hz, sz, hr, sr, xw, wp, ys, gt, ps, pr, ow, r2s, r2, na, nb,
        kv, qd, ob, outb, local_sem, send_sem, recv_sem,
    ) = refs
    z, x, y, c = (lax.axis_index(n) for n in ("z", "x", "y", "c"))
    other = 1 - c

    def zat(d):
        return lax.rem(z + d + NZ, NZ)

    def xat(d):
        return lax.rem(x + d + NX, NX)

    def yat(d):
        return lax.rem(y + d, NY)

    def cat(d):
        return other if d else c

    peers = [(z, x, yat(dy), cat(dc)) for dy in range(NY) for dc in range(NC) if dy or dc]
    row_peers = [(z, xat(dx), y, cat(dc)) for dx in range(1, NX) for dc in range(NC)]
    far = [(zat(d), x, y, c) for d in (-4, -3, -2, -1, 1, 2, 3, 4)]
    barrier = pltpu.get_barrier_semaphore()
    everyone = peers + row_peers + far
    for device in everyone:
        pl.semaphore_signal(barrier, inc=1, device_id=device, device_id_type=MESH)

    links = Links(send_sem, recv_sem)
    loads = [pltpu.make_async_copy(src, dst, local_sem.at[n]) for n, (src, dst) in enumerate(zip(homes, staged))]
    early = (0, 4, 2, 9, 11)
    late = (5, 6, 7, 8, 1, 3, 10)
    for n in early + late:
        loads[n].start()
    partner = (z, x, y, other)
    my_rows = pl.multiple_of(64 * c + 16 * y, 16)

    for n in early:
        loads[n].wait()
    ids_ref[...] = doc_ref[...].astype(F32)
    for hh in range(2):
        for j in range(3):
            wp_ref[hh, :, HEAD * j : HEAD * j + HEAD] = proj_ref[j, :, HEAD * hh : HEAD * hh + HEAD]
    part[0:128] = nt(x_ref[...], sel_ref[0:RANK]).astype(BF16)
    part[128:160] = nt(sel_ref[RANK:], x_ref[...]).astype(BF16)
    xw[z, x] = wo_ref[...]
    ids[0, :, pl.ds(pl.multiple_of(128 * x, 128), 128)] = ids_ref[...]
    pl.semaphore_wait(barrier, len(everyone))

    slot_pair, slot_rs = links.slots(1), links.slots(1)
    links.start(part, parts.at[0], partner, slot_pair)

    slot_i1 = links.slots(1)
    row_part = pl.ds(pl.multiple_of(128 * x, 128), 128)
    for dx in range(1, NX):
        links.start(ids_ref, ids.at[0, :, row_part], (z, xat(dx), y, c), slot_i1, 2)
    slot_x0 = links.slots(1)
    for hh in range(2):
        links.start(wp_ref.at[hh], wp.at[z, x], (z, 2 * c + hh, y, 1 - x // 2), slot_x0)

    slot_wo, slot_wp = links.slots(4), links.slots(4)
    ringed = pl.ds(pl.multiple_of(2 * other, 2), 2)

    def ring_out(phase):
        for sign in (1, -1):
            block = zat(-sign * 2 * (phase - 1))
            for near in (1, 2):
                far_by = sign * (2 * (phase - 1) + near)
                if far_by != -8:
                    links.start(
                        wo_ref if phase == 1 else xw.at[block, x],
                        xw.at[block, x],
                        (zat(sign * near), x, y, c),
                        slot_wo + phase - 1,
                    )

    def ring_proj(phase):
        for sign in (1, -1):
            block = zat(-sign * 2 * (phase - 1))
            for near in (1, 2):
                far_by = sign * (2 * (phase - 1) + near)
                if far_by != -8:
                    links.start(
                        wp.at[block, ringed],
                        wp.at[block, ringed],
                        (zat(sign * near), x, y, c),
                        slot_wp + phase - 1,
                    )

    def ring_wait(phase):
        links.wait(xw.at[0 : 4 - phase // 4, x], slot_wo + phase - 1, partner)

    def ring_proj_wait(phase):
        links.wait(wp.at[0 : 4 - phase // 4, ringed], slot_wp + phase - 1, partner)

    groups = [[0, -1, 1, -2, 2], [-3, 3, -4, 4], [-5, 5, -6, 6], [-7, 7, 8]]
    slot_near, slot_last = [links.slots(1) for _ in groups], [links.slots(1) for _ in range(2)]

    def spread(g, members):
        for d in members:
            piece = xw.at[zat(-d), x]
            for dx in (1, 3) if g < 2 else (2, 1, 3):
                links.start(piece, piece, (z, xat(dx), y, c), slot_near[g])

    def relay(g):
        links.wait(xw.at[0 : 2 * len(groups[g]), x], slot_near[g], partner)
        middle = (len(groups[g]) + 1) // 2
        for n, d in enumerate(groups[g]):
            toward = 1 if n < middle else -1
            piece = xw.at[zat(-d), xat(-toward)]
            links.start(piece, piece, (z, xat(toward), y, c), slot_last[g])

    def arrived(g):
        if g < 2:
            links.wait(xw.at[0 : len(groups[g]), x], slot_last[g], partner)
        else:
            links.wait(xw.at[0 : 3 * len(groups[g]), x], slot_near[g], partner)

    ring_out(1)
    spread(0, groups[0][:1])
    links.wait(parts.at[0], slot_pair, partner)
    selected = part[...].astype(F32) + parts[0].astype(F32)
    part2[...] = selected.astype(BF16)
    for dy in range(1, NY):
        links.start(part2, parts.at[dy], (z, x, yat(dy), c), slot_rs)
    for n in late:
        loads[n].wait()
    links.wait(ids.at[0, :, 0:384], slot_i1, partner)
    slot_i2 = links.slots(2)
    for dz in range(1, 5):
        links.start(ids.at[0], ids.at[dz], (zat(dz), x, y, c), slot_i2 + min(dz - 1, 1), 6)

    links.wait(wp.at[z, 0:2], slot_x0, partner)
    ring_wait(1)
    ring_out(2)
    spread(0, groups[0][1:])
    ring_proj(1)
    links.wait(parts.at[1:4], slot_rs, partner)
    for k in range(1, NY):
        selected = selected + parts[k].astype(F32)
    values = x_ref[...].astype(F32)
    step = softplus(nn(selected[:RANK].astype(BF16), stepw_ref[...]) + bias_ref[...])
    column = jnp.transpose(jnp.broadcast_to(ids_ref[...], (128, 128)))
    before = pltpu.roll(column, 1, axis=0)
    linked = (column == before) | (iota((128, 128), 0) == 0)
    for k in range(4):
        cols = slice(128 * k, 128 * k + 128)
        dt2[:, cols] = jnp.where(linked, step[:, cols], RESET)
    ss[x] = jnp.sum(dt2[...], axis=0, keepdims=True)
    slot_ss = links.slots(1)
    for dx in range(1, NX):
        links.start(ss.at[x], ss.at[x], (z, xat(dx), y, c), slot_ss, 4)

    driven = (step * values).astype(BF16)
    inputs = jnp.concatenate([selected[RANK : RANK + STATE]] * 16, axis=0)
    for k in range(8):
        token = iota((256, 128), 0) // STATE + k * 16
        spread_in = jnp.where(iota((256, 128), 1) == token, inputs, 0.0).astype(BF16)
        bx[256 * k : 256 * k + 256, :] = nn(spread_in, driven)
    rate = -jnp.exp(a_ref[...]) * LOG2E

    def scan(initial, keep_states):
        def advance(k, h):
            steps = dt2[pl.ds(pl.multiple_of(k * 8, 8), 8), :]
            for j in range(8):
                at = pl.ds(pl.multiple_of(k * 128 + j * 16, 16), 16)
                h = jnp.exp2(rate * steps[j : j + 1, :]) * h + bx[at, :]
                if keep_states:
                    hb[at, :] = h.astype(BF16)
            return h

        return lax.fori_loop(0, 16, advance, initial)

    hs[x] = scan(jnp.zeros((STATE, 512), F32), False).astype(BF16)
    slot_hs = links.slots(1)
    for dx in range(1, NX):
        links.start(hs.at[x], hs.at[x], (z, xat(dx), y, c), slot_hs)
    ring_wait(2)
    ring_out(3)
    spread(1, groups[1])
    relay(0)
    links.wait(ss.at[0:3], slot_ss, partner)
    links.wait(hs.at[0:3], slot_hs, partner)
    links.wait(ids.at[1], slot_i2, partner)
    prior = jnp.where(z == 0, -1.0, ids[1, :, 511:512])
    breaks = []
    for k in range(NX):
        if k:
            prior = ids[0, :, 128 * k - 1 : 128 * k]
        first = ids[0, :, 128 * k : 128 * k + 1]
        breaks.append(jnp.broadcast_to(jnp.where(first == prior, 0.0, RESET), (1, 512)))
    running = jnp.zeros((STATE, 512), F32)
    steps_sum = jnp.zeros((1, 512), F32)
    own_prior, own_steps, own_break = running, steps_sum, steps_sum
    for k in range(NX):
        own_prior = jnp.where(x == k, running, own_prior)
        own_steps = jnp.where(x == k, steps_sum, own_steps)
        own_break = jnp.where(x == k, breaks[k], own_break)
        steps_of = ss[k] + breaks[k]
        running = jnp.exp2(rate * steps_of) * running + hs[k].astype(F32)
        steps_sum = steps_sum + steps_of
    dt2[0:1, :] = dt2[0:1, :] + own_break
    hr[...] = running.astype(BF16)
    sr[...] = steps_sum
    slot_hz, slot_sz = links.slots(1), links.slots(1)
    for dz in range(1, 5):
        links.start(hr, hz.at[dz - 1], (zat(dz), x, y, c), slot_hz)
        links.start(sr, sz.at[dz - 1], (zat(dz), x, y, c), slot_sz, 5)
    ring_wait(3)
    ring_out(4)
    relay(1)
    spread(2, groups[2])
    links.wait(hz, slot_hz, partner)
    links.wait(sz, slot_sz, partner)
    above = jnp.zeros((STATE, 512), F32)
    for dz in range(4, 0, -1):
        joined = jnp.exp2(rate * sz[dz - 1]) * above + hz[dz - 1].astype(F32)
        above = jnp.where(z >= dz, joined, jnp.zeros_like(joined))
    carry = jnp.exp2(rate * own_steps) * above + own_prior
    ring_proj_wait(1)
    ring_proj(2)
    scan(carry, True)
    ring_wait(4)
    spread(3, groups[3])
    pick_out = (lax.rem(iota((STATE, 256), 1), STATE) == iota((STATE, 256), 0)).astype(BF16)
    coefs = lax.dot_general(
        selected[RANK + STATE :].astype(BF16), pick_out, (((0,), (0,)), ((), ())), preferred_element_type=F32
    )
    own_token = iota((16, 256), 1) // STATE == iota((16, 256), 0)

    for k in range(8):
        rows = slice(16 * k, 16 * k + 16)
        coef = jnp.where(own_token, coefs[rows], 0.0).astype(BF16)
        ys[rows, :] = nn(coef, hb[256 * k : 256 * k + 256, :])
    gate = g_ref[...].astype(F32)
    mixed = (ys[...] + skip_ref[...] * values) * (gate / (1.0 + jnp.exp(-gate)))
    gt[...] = mixed.astype(BF16)

    slot_pr = [links.slots(1) for _ in groups]
    slot_r2 = [links.slots(1) for _ in groups]
    half_rows = pl.ds(pl.multiple_of(64 * c, 64), 64)
    their_rows = pl.ds(pl.multiple_of(64 * other, 64), 64)

    def columns(d):
        return pl.ds(pl.multiple_of(128 * zat(-d), 128), 128)

    def weight_of(d):
        return xw[zat(-d)].reshape(128, 512)

    def project_pair(g):
        for d in groups[g]:
            ps[:, columns(d)] = nt(gt[their_rows, :], weight_of(d)).astype(BF16)
        for d in groups[g]:
            piece = ps.at[:, columns(d)]
            links.start(piece, pr.at[:, columns(d)], partner, slot_pr[g])

    def project_own(g):
        for d in groups[g]:
            ow[:, columns(d)] = nt(gt[half_rows, :], weight_of(d))
        width = 128 * len(groups[g])
        links.wait(pr.at[:, 0:width], slot_pr[g], partner)
        for d in groups[g]:
            joined = ow[:, columns(d)] + pr[:, columns(d)].astype(F32)
            ow[:, columns(d)] = joined
            r2s[:, columns(d)] = joined.astype(BF16)
        for d in groups[g]:
            for dy in range(1, NY):
                ty = yat(dy)
                piece = r2s.at[pl.ds(pl.multiple_of(16 * ty, 16), 16), columns(d)]
                links.start(piece, r2.at[dy, :, columns(d)], (z, x, ty, c), slot_r2[g], 1)

    arrived(0)
    project_pair(0)
    arrived(1)
    project_pair(1)
    project_own(0)
    project_own(1)
    arrived(2)
    project_pair(2)
    project_own(2)
    ring_proj_wait(2)
    ring_proj(3)
    arrived(3)
    project_pair(3)
    project_own(3)
    stream = ow[pl.ds(pl.multiple_of(16 * y, 16), 16), :] + res_ref[pl.ds(my_rows, 16), :].astype(F32)
    for g in range(len(groups)):
        width = 128 * len(groups[g])
        links.wait(r2.at[0:3, :, 0:width], slot_r2[g], partner)
    for dy in range(1, NY):
        stream = stream + r2[dy].astype(F32)
    links.wait(ids.at[2:5], slot_i2 + 1, partner)
    stream = stream.astype(BF16).astype(F32)
    normed = stream * lax.rsqrt(jnp.mean(stream * stream, axis=-1, keepdims=True) + EPS) * gain_ref[...]
    normed = normed.astype(BF16)

    na[x, y] = normed[:, :1024]
    nb[x, y] = normed[:, 1024:]
    slot_n1, slot_n2 = links.slots(3), links.slots(3)
    slot_n3, slot_n4 = links.slots(1), links.slots(1)
    for d in range(1, 4):
        links.start(na.at[x, y], na.at[x, y], (z, xat(d), y, c), slot_n1 + d - 1)
        links.start(nb.at[x, y], nb.at[x, y], (z, x, yat(d), c), slot_n2 + d - 1)

    def over_y(k):
        piece = na.at[xat(k), y]
        for d in range(1, 4):
            links.start(piece, piece, (z, x, yat(d), c), slot_n3)

    def over_x(k):
        piece = nb.at[x, yat(k)]
        for d in range(1, 4):
            links.start(piece, piece, (z, xat(d), y, c), slot_n4)

    over_y(0)
    over_x(0)
    ring_proj_wait(3)
    ring_proj(4)

    for k in range(NX):
        qd[k] = jnp.transpose(jnp.broadcast_to(ids[0, :, 128 * k : 128 * k + 128], (128, 128)))
    q_doc = jnp.concatenate([qd[k, half_rows, :] for k in range(NX)], axis=0)
    row_of = iota((256, 128), 0)
    in_row = 128 * (row_of // 64) + 64 * c + lax.rem(row_of, 64)
    for k in (3, 1, 2):
        links.wait(na.at[x, y], slot_n1 + 3 - k, partner)
        over_y(k)
        links.wait(nb.at[x, y], slot_n2 + 3 - k, partner)
        over_x(k)
    ring_proj_wait(4)
    slot_pw = links.slots(1)
    links.start(wp.at[:, ringed], wp.at[:, ringed], partner, slot_pw)

    slot_kz = [None] + [links.slots(4) for _ in range(4)]
    slot_kc = links.slots(5)

    def chunk(d, k, core):
        return kv.at[d, xat(k), core]

    def pass_on(d, k):
        if d < 4:
            links.start(chunk(d, k, c), chunk(d + 1, k, c), (zat(1), x, y, c), slot_kz[d + 1] + k)
        links.start(chunk(d, k, c), chunk(d, k, c), partner, slot_kc + d)

    def forward(d, k):
        links.wait(chunk(d, k, c), slot_kz[d] + k, partner)
        pass_on(d, k)

    links.wait(na.at[0:3], slot_n3, partner)
    links.wait(nb.at[0:3], slot_n4, partner)
    links.wait(wp.at[:, ringed], slot_pw, partner)
    made = nn(na[...].reshape(256, 1024), wp[0:8].reshape(1024, 384))
    made = made + nn(nb[...].reshape(256, 1024), wp[8:16].reshape(1024, 384))
    query = made[:, :HEAD].astype(BF16)
    kv[0, :, c] = made[:, HEAD:].astype(BF16).reshape(4, 64, 256)
    for k in range(4):
        pass_on(0, k)

    def attend(d, carried, blocks):
        top, mass, acc = carried
        links.wait(kv.at[d, :, other], slot_kc + d, partner)
        scores, places = [], []
        for k in blocks:
            place = xat(k)
            piece = nt(query, kv[d, place, :, :, :HEAD].reshape(128, HEAD)) * (HEAD**-0.5 * LOG2E)
            k_doc = jnp.where(z >= d, ids[d, :, pl.ds(pl.multiple_of(128 * place, 128), 128)], -1.0)
            allowed = jnp.broadcast_to(k_doc, (256, 128)) == q_doc
            ahead = iota((256, 128), 1) + 128 * place - in_row
            if d == 0:
                allowed = allowed & (ahead <= 0)
            if d == 4:
                allowed = allowed & (ahead > 0)
            scores.append(jnp.where(allowed, piece, HIDDEN))
            places.append(place)
        highest = scores[0]
        for piece in scores[1:]:
            highest = jnp.maximum(highest, piece)
        new_top = jnp.maximum(top, jnp.max(highest, axis=-1, keepdims=True))
        shrink = jnp.exp2(top - new_top)
        acc = acc * shrink
        added = jnp.zeros((256, 128), F32)
        for place, piece in zip(places, scores):
            probs = jnp.exp2(piece - new_top)
            added = added + probs
            acc = acc + nn(probs.astype(BF16), kv[d, place, :, :, HEAD:].reshape(128, HEAD))
        mass = mass * shrink + jnp.sum(added, axis=-1, keepdims=True)
        return new_top, mass, acc

    carried = (jnp.full((256, 1), HIDDEN, F32), jnp.zeros((256, 1), F32), jnp.zeros((256, HEAD), F32))
    every = (0, 1, 2, 3)
    carried = attend(0, carried, every)
    for d in range(1, 4):
        for k in range(4):
            forward(d, k)
        if d > 1:
            carried = attend(d - 1, carried, every)
    forward(4, 0)
    forward(4, 1)
    carried = attend(3, carried, every)
    forward(4, 2)
    forward(4, 3)
    top, mass, acc = attend(4, carried, every)
    ob[...] = (acc / mass).astype(BF16).reshape(4, 64, HEAD)

    slot_o = links.slots(4)
    mine = slot_o + lax.rem(x, 2) * 2 + c
    cols = pl.ds(pl.multiple_of(128 * lax.rem(x, 2), 128), 128)
    for dx in range(1, NX):
        tx = xat(dx)
        links.start(ob.at[tx], outb.at[half_rows, cols], (z, tx, y, x // 2), mine)
    stays = c == x // 2
    to_partner = links.copy(ob.at[x], outb.at[half_rows, cols], partner, mine, 3)

    @pl.when(stays)
    def _():
        outb[half_rows, cols] = ob[x]

    @pl.when(jnp.logical_not(stays))
    def _():
        to_partner.start()

    for k in range(4):
        from_me = stays & (lax.rem(x, 2) * 2 + c == k)

        @pl.when(jnp.logical_not(from_me))
        def _():
            links.wait(outb.at[half_rows, cols], slot_o + k, partner)

    out_ref[...] = outb[...]

    @pl.when(jnp.logical_not(stays))
    def _():
        to_partner.wait_send()

    for send in range(2):
        assert links.sent[send] % 16384 == 0
        links.drain(send, bx.at[0 : links.sent[send] // 2048], partner)
    links.drain(2, ids.at[0, :, 0:384], partner)
    links.drain(4, ss.at[0:3], partner)
    links.drain(5, sz, partner)
    links.drain(6, ids.at[0:4], partner)
    assert links.recvs <= RECVS, links.recvs


SENDS, RECVS = 7, 68
SEND_MOST = 4 << 20


def body(
    mixer_input, gate_input, document_ids, residual, select_weight, step_weight, step_bias, decay_log, skip_gain,
    out_weight, norm_gain, project_weight,
):
    vmem = pl.BlockSpec(memory_space=pltpu.VMEM)
    hbm = pl.BlockSpec(memory_space=pltpu.HBM)
    operands = (
        mixer_input,
        gate_input,
        document_ids.reshape(1, 128),
        residual,
        select_weight.T,
        step_weight,
        step_bias.reshape(1, 512),
        decay_log.T,
        skip_gain.reshape(1, 512),
        out_weight.T,
        norm_gain.reshape(1, 2048),
        project_weight.transpose(1, 0, 2),
    )
    scratch = [pltpu.VMEM(o.shape, o.dtype) for o in operands]
    scratch += [
        pltpu.VMEM((160, 128), BF16),
        pltpu.VMEM((160, 128), BF16),
        pltpu.VMEM((4, 160, 128), BF16),
        pltpu.VMEM((1, 128), F32),
        pltpu.VMEM((2, 32, 384), BF16),
        pltpu.VMEM((5, 1, 512), F32),
        pltpu.VMEM((128, 512), F32),
        pltpu.VMEM((2048, 512), F32),
        pltpu.VMEM((2048, 512), BF16),
        pltpu.VMEM((4, 16, 512), BF16),
        pltpu.VMEM((4, 1, 512), F32),
        pltpu.VMEM((4, 16, 512), BF16),
        pltpu.VMEM((4, 1, 512), F32),
        pltpu.VMEM((16, 512), BF16),
        pltpu.VMEM((1, 512), F32),
        pltpu.VMEM((16, 4, 32, 512), BF16),
        pltpu.VMEM((16, 4, 32, 384), BF16),
        pltpu.VMEM((128, 512), F32),
        pltpu.VMEM((128, 512), BF16),
        pltpu.VMEM((64, 2048), BF16),
        pltpu.VMEM((64, 2048), BF16),
        pltpu.VMEM((64, 2048), F32),
        pltpu.VMEM((64, 2048), BF16),
        pltpu.VMEM((4, 16, 2048), BF16),
        pltpu.VMEM((4, 4, 16, 1024), BF16),
        pltpu.VMEM((4, 4, 16, 1024), BF16),
        pltpu.VMEM((5, 4, 2, 64, 256), BF16),
        pltpu.VMEM((4, 128, 128), F32),
        pltpu.VMEM((4, 64, 128), BF16),
        pltpu.VMEM((128, 256), BF16),
        pltpu.SemaphoreType.DMA((12,)),
        pltpu.SemaphoreType.DMA((SENDS,)),
        pltpu.SemaphoreType.DMA((RECVS,)),
    ]
    return pl.pallas_call(
        kernel,
        out_shape=jax.ShapeDtypeStruct((128, 256), BF16),
        in_specs=[hbm] * len(operands),
        out_specs=vmem,
        scratch_shapes=scratch,
        compiler_params=pltpu.CompilerParams(collective_id=0, has_side_effects=True, vmem_limit_bytes=48 << 20),
    )(*[pltpu.with_memory_space_constraint(o, pltpu.HBM) for o in operands])


def solution(mesh):
    split = Mesh(mesh.devices.reshape(NZ, NX, NY, NC), ("z", "x", "y", "c"))
    placed = (
        P(SEQ, TP), P(SEQ, TP), P(SEQ), P(SEQ, None), P(TP, None), P(None, TP), P(TP), P(TP, None), P(TP),
        P(TP, SEQ), P(), P(SEQ, None, TP),
    )
    return jax.shard_map(body, mesh=split, in_specs=placed, out_specs=P(SEQ, TP), check_vma=False)
```

```python
import math

import jax
import jax.numpy as jnp
from jax import lax
from jax.experimental import pallas as pl
from jax.experimental.pallas import tpu as pltpu
from jax.sharding import Mesh
from jax.sharding import PartitionSpec as P

MESH = pl.DeviceIdType.MESH
NZ, NX, NY, NC = 16, 4, 4, 2
STATE = 16
RANK = 128
HEAD = 128
WINDOW = 2048
EPS = 1e-05
LOG2E = 1.4426950408889634
RESET = 1e6
HIDDEN = -1e30
SEQ = ("z", "x")
TP = ("y", "c")
F32 = jnp.float32
BF16 = jnp.bfloat16


def nt(a, b):
    return lax.dot_general(a, b, (((1,), (1,)), ((), ())), preferred_element_type=F32)


def nn(a, b):
    return jnp.dot(a, b, preferred_element_type=F32)


def iota(shape, dim):
    return lax.broadcasted_iota(jnp.int32, shape, dim)


def softplus(v):
    e = jnp.exp(-jnp.abs(v))
    small = e * (1.0 - e * (0.5 - e * (1.0 / 3.0 - e * 0.25)))
    return jnp.maximum(v, 0.0) + jnp.where(e < 0.01, small, jnp.log(1.0 + e))


class Links:
    def __init__(self, send, recv):
        self.send, self.recv = send, recv
        self.recvs = 0
        self.sent = [0] * SENDS

    def slots(self, count):
        first = self.recvs
        self.recvs += count
        return first

    def copy(self, src, dst, device, slot, send):
        return pltpu.make_async_remote_copy(
            src_ref=src,
            dst_ref=dst,
            send_sem=self.send.at[send],
            recv_sem=self.recv.at[slot],
            device_id=device,
            device_id_type=MESH,
        )

    def start(self, src, dst, device, slot, send=None):
        size = math.prod(src.shape) * jnp.dtype(src.dtype).itemsize
        if send is None:
            send = 0 if self.sent[0] + size <= SEND_MOST else 1
        self.sent[send] += size
        self.copy(src, dst, device, slot, send).start()

    def wait(self, dst, slot, device):
        self.copy(dst, dst, device, slot, 0).wait_recv()

    def drain(self, send, whole, device):
        self.copy(whole, whole, device, 0, send).wait_send()


def kernel(
    *refs
):
    homes, refs = refs[:12], refs[12:]
    out_ref, refs = refs[0], refs[1:]
    staged, refs = refs[:12], refs[12:]
    x_ref, g_ref, doc_ref, res_ref, sel_ref, stepw_ref, bias_ref, a_ref, skip_ref, wo_ref, gain_ref, proj_ref = staged
    (
        part, part2, parts, ids_ref, wp_ref, ids, dt2, bx, hb, hs, ss, hz, sz, hr, sr, xw, wp, ys, gt, ps, pr, pf, r2s, r2, p3, f3, r3, na, nb,
        kv, qd, ob, outb, local_sem, send_sem, recv_sem,
    ) = refs
    z, x, y, c = (lax.axis_index(n) for n in ("z", "x", "y", "c"))
    other = 1 - c

    def zat(d):
        return lax.rem(z + d + NZ, NZ)

    def xat(d):
        return lax.rem(x + d + NX, NX)

    def yat(d):
        return lax.rem(y + d, NY)

    def cat(d):
        return other if d else c

    peers = [(z, x, yat(dy), cat(dc)) for dy in range(NY) for dc in range(NC) if dy or dc]
    row_peers = [(z, xat(dx), y, cat(dc)) for dx in range(1, NX) for dc in range(NC)]
    far = [(zat(d), x, y, c) for d in (-4, -3, -2, -1, 1, 2, 3, 4)]
    barrier = pltpu.get_barrier_semaphore()
    everyone = peers + row_peers + far
    for device in everyone:
        pl.semaphore_signal(barrier, inc=1, device_id=device, device_id_type=MESH)

    links = Links(send_sem, recv_sem)
    groups = [[0, -1, 1, -2, 2], [-3, 3, -4, 4], [-5, 5, -6, 6], [-7, 7, 8]]

    def columns(d):
        return pl.ds(pl.multiple_of(128 * zat(-d), 128), 128)

    loads = [pltpu.make_async_copy(src, dst, local_sem.at[n]) for n, (src, dst) in enumerate(zip(homes, staged))]
    early = (0, 4, 2, 9, 11)
    late = (5, 6, 7, 8, 1, 3, 10)
    for n in early + late:
        loads[n].start()
    partner = (z, x, y, other)
    my_rows = pl.multiple_of(64 * c + 16 * y, 16)

    for n in early:
        loads[n].wait()
    ids_ref[...] = doc_ref[...].astype(F32)
    for hh in range(2):
        for j in range(3):
            wp_ref[hh, :, HEAD * j : HEAD * j + HEAD] = proj_ref[j, :, HEAD * hh : HEAD * hh + HEAD]
    part[0:128] = nt(x_ref[...], sel_ref[0:RANK]).astype(BF16)
    part[128:160] = nt(sel_ref[RANK:], x_ref[...]).astype(BF16)
    xw[z, x] = wo_ref[...]
    ids[0, :, pl.ds(pl.multiple_of(128 * x, 128), 128)] = ids_ref[...]
    for d in groups[3]:
        r2[:, :, columns(d)] = jnp.zeros((4, 16, 128), BF16)
    pl.semaphore_wait(barrier, len(everyone))

    slot_pair, slot_rs = links.slots(1), links.slots(1)
    links.start(part, parts.at[0], partner, slot_pair)

    slot_i1 = links.slots(1)
    row_part = pl.ds(pl.multiple_of(128 * x, 128), 128)
    for dx in range(1, NX):
        links.start(ids_ref, ids.at[0, :, row_part], (z, xat(dx), y, c), slot_i1, 2)
    slot_x0 = links.slots(1)
    for hh in range(2):
        links.start(wp_ref.at[hh], wp.at[z, x], (z, 2 * c + hh, y, 1 - x // 2), slot_x0)

    slot_wo, slot_wp = links.slots(8), links.slots(4)
    ringed = pl.ds(pl.multiple_of(2 * other, 2), 2)

    def ring_out(phase):
        for near in (2, 1):
            for sign in (1, -1):
                block = zat(-sign * 2 * (phase - 1))
                if sign * (2 * (phase - 1) + near) != -8:
                    links.start(
                        wo_ref if phase == 1 else xw.at[block, x],
                        xw.at[block, x],
                        (zat(sign * near), x, y, c),
                        slot_wo + 2 * phase - near,
                    )

    def ring_proj(phase):
        for sign in (1, -1):
            block = zat(-sign * 2 * (phase - 1))
            for near in (1, 2):
                far_by = sign * (2 * (phase - 1) + near)
                if far_by != -8:
                    links.start(
                        wp.at[block, ringed],
                        wp.at[block, ringed],
                        (zat(sign * near), x, y, c),
                        slot_wp + phase - 1,
                    )

    def ring_far(phase):
        links.wait(xw.at[0 : 2 - phase // 4, x], slot_wo + 2 * phase - 2, partner)

    def ring_near(phase):
        links.wait(xw.at[0:2, x], slot_wo + 2 * phase - 1, partner)

    def ring_proj_wait(phase):
        links.wait(wp.at[0 : 4 - phase // 4, ringed], slot_wp + phase - 1, partner)

    slot_near, slot_last = [links.slots(1) for _ in groups], [links.slots(1) for _ in range(2)]

    def spread(g, members):
        for d in members:
            piece = xw.at[zat(-d), x]
            for dx in (1, 3) if g < 2 else (2, 1, 3):
                links.start(piece, piece, (z, xat(dx), y, c), slot_near[g])

    def relay(g):
        links.wait(xw.at[0 : 2 * len(groups[g]), x], slot_near[g], partner)
        middle = (len(groups[g]) + 1) // 2
        for n, d in enumerate(groups[g]):
            toward = 1 if n < middle else -1
            piece = xw.at[zat(-d), xat(-toward)]
            links.start(piece, piece, (z, xat(toward), y, c), slot_last[g])

    def arrived(g):
        if g < 2:
            links.wait(xw.at[0 : len(groups[g]), x], slot_last[g], partner)
        else:
            links.wait(xw.at[0 : 3 * len(groups[g]), x], slot_near[g], partner)

    ring_out(1)
    spread(0, groups[0][:1])
    links.wait(parts.at[0], slot_pair, partner)
    selected = part[...].astype(F32) + parts[0].astype(F32)
    part2[...] = selected.astype(BF16)
    for dy in range(1, NY):
        links.start(part2, parts.at[dy], (z, x, yat(dy), c), slot_rs)
    for n in late:
        loads[n].wait()
    links.wait(ids.at[0, :, 0:384], slot_i1, partner)
    slot_i2 = links.slots(2)
    for dz in range(1, 5):
        links.start(ids.at[0], ids.at[dz], (zat(dz), x, y, c), slot_i2 + min(dz - 1, 1), 6)

    ring_far(1)
    ring_out(2)
    ring_near(1)
    spread(0, groups[0][1:])
    links.wait(wp.at[z, 0:2], slot_x0, partner)
    ring_proj(1)
    links.wait(parts.at[1:4], slot_rs, partner)
    for k in range(1, NY):
        selected = selected + parts[k].astype(F32)
    values = x_ref[...].astype(F32)
    step = softplus(nn(selected[:RANK].astype(BF16), stepw_ref[...]) + bias_ref[...])
    column = jnp.transpose(jnp.broadcast_to(ids_ref[...], (128, 128)))
    before = pltpu.roll(column, 1, axis=0)
    linked = (column == before) | (iota((128, 128), 0) == 0)
    for k in range(4):
        cols = slice(128 * k, 128 * k + 128)
        dt2[:, cols] = jnp.where(linked, step[:, cols], RESET)
    ss[x] = jnp.sum(dt2[...], axis=0, keepdims=True)
    slot_ss = links.slots(1)
    for dx in range(1, NX):
        links.start(ss.at[x], ss.at[x], (z, xat(dx), y, c), slot_ss, 4)

    driven = (step * values).astype(BF16)
    inputs = jnp.concatenate([selected[RANK : RANK + STATE]] * 16, axis=0)
    for k in range(8):
        token = iota((256, 128), 0) // STATE + k * 16
        spread_in = jnp.where(iota((256, 128), 1) == token, inputs, 0.0).astype(BF16)
        bx[256 * k : 256 * k + 256, :] = nn(spread_in, driven)
    rate = -jnp.exp(a_ref[...]) * LOG2E

    def scan(initial, keep_states):
        def advance(k, h):
            steps = dt2[pl.ds(pl.multiple_of(k * 8, 8), 8), :]
            for j in range(8):
                at = pl.ds(pl.multiple_of(k * 128 + j * 16, 16), 16)
                h = jnp.exp2(rate * steps[j : j + 1, :]) * h + bx[at, :]
                if keep_states:
                    hb[at, :] = h.astype(BF16)
            return h

        return lax.fori_loop(0, 16, advance, initial)

    hs[x] = scan(jnp.zeros((STATE, 512), F32), False).astype(BF16)
    slot_hs = links.slots(1)
    for dx in range(1, NX):
        links.start(hs.at[x], hs.at[x], (z, xat(dx), y, c), slot_hs)
    ring_far(2)
    ring_out(3)
    ring_near(2)
    spread(1, groups[1])
    relay(0)
    links.wait(ss.at[0:3], slot_ss, partner)
    links.wait(hs.at[0:3], slot_hs, partner)
    links.wait(ids.at[1], slot_i2, partner)
    prior = jnp.where(z == 0, -1.0, ids[1, :, 511:512])
    breaks = []
    for k in range(NX):
        if k:
            prior = ids[0, :, 128 * k - 1 : 128 * k]
        first = ids[0, :, 128 * k : 128 * k + 1]
        breaks.append(jnp.broadcast_to(jnp.where(first == prior, 0.0, RESET), (1, 512)))
    running = jnp.zeros((STATE, 512), F32)
    steps_sum = jnp.zeros((1, 512), F32)
    own_prior, own_steps, own_break = running, steps_sum, steps_sum
    for k in range(NX):
        own_prior = jnp.where(x == k, running, own_prior)
        own_steps = jnp.where(x == k, steps_sum, own_steps)
        own_break = jnp.where(x == k, breaks[k], own_break)
        steps_of = ss[k] + breaks[k]
        running = jnp.exp2(rate * steps_of) * running + hs[k].astype(F32)
        steps_sum = steps_sum + steps_of
    dt2[0:1, :] = dt2[0:1, :] + own_break
    hr[...] = running.astype(BF16)
    sr[...] = steps_sum
    slot_hz, slot_sz = links.slots(1), links.slots(1)
    for dz in range(1, 5):
        links.start(hr, hz.at[dz - 1], (zat(dz), x, y, c), slot_hz)
        links.start(sr, sz.at[dz - 1], (zat(dz), x, y, c), slot_sz, 5)
    ring_far(3)
    ring_out(4)
    ring_near(3)
    relay(1)
    spread(2, groups[2])
    ring_far(4)
    ring_near(4)
    spread(3, groups[3])
    links.wait(hz, slot_hz, partner)
    links.wait(sz, slot_sz, partner)
    above = jnp.zeros((STATE, 512), F32)
    for dz in range(4, 0, -1):
        joined = jnp.exp2(rate * sz[dz - 1]) * above + hz[dz - 1].astype(F32)
        above = jnp.where(z >= dz, joined, jnp.zeros_like(joined))
    carry = jnp.exp2(rate * own_steps) * above + own_prior
    ring_proj_wait(1)
    ring_proj(2)
    scan(carry, True)
    pick_out = (lax.rem(iota((STATE, 256), 1), STATE) == iota((STATE, 256), 0)).astype(BF16)
    coefs = lax.dot_general(
        selected[RANK + STATE :].astype(BF16), pick_out, (((0,), (0,)), ((), ())), preferred_element_type=F32
    )
    own_token = iota((16, 256), 1) // STATE == iota((16, 256), 0)

    for k in range(8):
        rows = slice(16 * k, 16 * k + 16)
        coef = jnp.where(own_token, coefs[rows], 0.0).astype(BF16)
        ys[rows, :] = nn(coef, hb[256 * k : 256 * k + 256, :])
    gate = g_ref[...].astype(F32)
    mixed = (ys[...] + skip_ref[...] * values) * (gate / (1.0 + jnp.exp(-gate)))
    gt[...] = mixed.astype(BF16)

    slot_pr = [links.slots(1) for _ in groups]
    slot_r2 = [links.slots(1) for _ in groups]
    half_rows = pl.ds(pl.multiple_of(64 * c, 64), 64)
    their_rows = pl.ds(pl.multiple_of(64 * other, 64), 64)

    def weight_of(d):
        return xw[zat(-d)].reshape(128, 512)

    def project(g):
        for d in groups[g]:
            pf[:, columns(d)] = nt(gt[...], weight_of(d))
        for d in groups[g]:
            ps[:, columns(d)] = pf[their_rows, columns(d)].astype(BF16)
            links.start(ps.at[:, columns(d)], pr.at[:, columns(d)], partner, slot_pr[g])

    def finish(g):
        width = 128 * len(groups[g])
        links.wait(pr.at[:, 0:width], slot_pr[g], partner)
        for d in groups[g]:
            joined = pf[half_rows, columns(d)] + pr[:, columns(d)].astype(F32)
            pf[half_rows, columns(d)] = joined
            r2s[:, columns(d)] = joined.astype(BF16)
        for d in groups[g]:
            for dy in range(1, NY):
                ty = yat(dy)
                piece = r2s.at[pl.ds(pl.multiple_of(16 * ty, 16), 16), columns(d)]
                links.start(piece, r2.at[dy, :, columns(d)], (z, x, ty, c), slot_r2[g], 8)

    arrived(0)
    project(0)
    arrived(1)
    project(1)
    finish(0)
    arrived(2)
    project(2)
    finish(1)
    ring_proj_wait(2)
    ring_proj(3)
    finish(2)
    arrived(3)
    slot_r3 = links.slots(1)
    for j, d in enumerate(groups[3]):
        product = nt(gt[...], weight_of(d))
        f3[:, 128 * j : 128 * j + 128] = product
        p3[:, 128 * j : 128 * j + 128] = product.astype(BF16)
    for dy in range(NY):
        for dc in range(NC):
            if dy or dc:
                ty, tc = yat(dy), cat(dc)
                rows = pl.ds(pl.multiple_of(64 * tc + 16 * ty, 16), 16)
                links.start(p3.at[rows], r3.at[dy * 2 + dc], (z, x, ty, tc), slot_r3, 7)
    for g in range(3):
        width = 128 * len(groups[g])
        links.wait(r2.at[0:3, :, 0:width], slot_r2[g], partner)
    links.wait(r3.at[1:8], slot_r3, partner)
    straight = f3[pl.ds(my_rows, 16), :]
    for k in range(1, 8):
        straight = straight + r3[k].astype(F32)
    for j, d in enumerate(groups[3]):
        pf[pl.ds(my_rows, 16), columns(d)] = straight[:, 128 * j : 128 * j + 128]
    stream = pf[pl.ds(my_rows, 16), :] + res_ref[pl.ds(my_rows, 16), :].astype(F32)
    for dy in range(1, NY):
        stream = stream + r2[dy].astype(F32)
    links.wait(ids.at[2:5], slot_i2 + 1, partner)
    stream = stream.astype(BF16).astype(F32)
    normed = stream * lax.rsqrt(jnp.mean(stream * stream, axis=-1, keepdims=True) + EPS) * gain_ref[...]
    normed = normed.astype(BF16)

    na[x, y] = normed[:, :1024]
    nb[x, y] = normed[:, 1024:]
    slot_n1, slot_n2 = links.slots(3), links.slots(3)
    slot_n3, slot_n4 = links.slots(1), links.slots(1)
    for d in range(1, 4):
        links.start(na.at[x, y], na.at[x, y], (z, xat(d), y, c), slot_n1 + d - 1)
        links.start(nb.at[x, y], nb.at[x, y], (z, x, yat(d), c), slot_n2 + d - 1)

    def over_y(k):
        piece = na.at[xat(k), y]
        for d in range(1, 4):
            links.start(piece, piece, (z, x, yat(d), c), slot_n3)

    def over_x(k):
        piece = nb.at[x, yat(k)]
        for d in range(1, 4):
            links.start(piece, piece, (z, xat(d), y, c), slot_n4)

    over_y(0)
    over_x(0)
    ring_proj_wait(3)
    ring_proj(4)

    for k in range(NX):
        qd[k] = jnp.transpose(jnp.broadcast_to(ids[0, :, 128 * k : 128 * k + 128], (128, 128)))
    q_doc = jnp.concatenate([qd[k, half_rows, :] for k in range(NX)], axis=0)
    row_of = iota((256, 128), 0)
    in_row = 128 * (row_of // 64) + 64 * c + lax.rem(row_of, 64)
    for k in (3, 1, 2):
        links.wait(na.at[x, y], slot_n1 + 3 - k, partner)
        over_y(k)
        links.wait(nb.at[x, y], slot_n2 + 3 - k, partner)
        over_x(k)
    ring_proj_wait(4)
    slot_pw = links.slots(1)
    links.start(wp.at[:, ringed], wp.at[:, ringed], partner, slot_pw)

    slot_kz = [None] + [links.slots(4) for _ in range(4)]
    slot_kc = links.slots(5)

    def chunk(d, k, core):
        return kv.at[d, xat(k), core]

    def pass_on(d, k):
        if d < 4:
            links.start(chunk(d, k, c), chunk(d + 1, k, c), (zat(1), x, y, c), slot_kz[d + 1] + k)
        links.start(chunk(d, k, c), chunk(d, k, c), partner, slot_kc + d)

    def forward(d, k):
        links.wait(chunk(d, k, c), slot_kz[d] + k, partner)
        pass_on(d, k)

    links.wait(na.at[0:3], slot_n3, partner)
    links.wait(nb.at[0:3], slot_n4, partner)
    links.wait(wp.at[:, ringed], slot_pw, partner)
    made = nn(na[...].reshape(256, 1024), wp[0:8].reshape(1024, 384))
    made = made + nn(nb[...].reshape(256, 1024), wp[8:16].reshape(1024, 384))
    query = made[:, :HEAD].astype(BF16)
    kv[0, :, c] = made[:, HEAD:].astype(BF16).reshape(4, 64, 256)
    for k in range(4):
        pass_on(0, k)

    def attend(d, half, carried):
        top, mass, acc = carried
        rows = slice(128 * half, 128 * half + 128)
        scores = []
        for k in range(NX):
            piece = nt(query[rows], kv[d, k, :, :, :HEAD].reshape(128, HEAD)) * (HEAD**-0.5 * LOG2E)
            k_doc = jnp.where(z >= d, ids[d, :, 128 * k : 128 * k + 128], -1.0)
            allowed = jnp.broadcast_to(k_doc, (128, 128)) == q_doc[rows]
            ahead = iota((128, 128), 1) + 128 * k - in_row[rows]
            if d == 0:
                allowed = allowed & (ahead <= 0)
            if d == 4:
                allowed = allowed & (ahead > 0)
            scores.append(jnp.where(allowed, piece, HIDDEN))
        highest = jnp.maximum(jnp.maximum(scores[0], scores[1]), jnp.maximum(scores[2], scores[3]))
        new_top = jnp.maximum(top, jnp.max(highest, axis=-1, keepdims=True))
        shrink = jnp.exp2(top - new_top)
        probs = [jnp.exp2(piece - new_top) for piece in scores]
        added = (probs[0] + probs[1]) + (probs[2] + probs[3])
        mass = mass * shrink + jnp.sum(added, axis=-1, keepdims=True)
        joined = jnp.concatenate([p.astype(BF16) for p in probs], axis=1)
        acc = acc * shrink + nn(joined, kv[d, :, :, :, HEAD:].reshape(512, HEAD))
        return new_top, mass, acc

    def shared(d):
        links.wait(kv.at[d, :, other], slot_kc + d, partner)

    start = (jnp.full((128, 1), HIDDEN, F32), jnp.zeros((128, 1), F32), jnp.zeros((128, HEAD), F32))
    shared(0)
    first, second = attend(0, 0, start), attend(0, 1, start)
    for k in range(4):
        forward(1, k)
    for d in range(2, 5):
        forward(d, 0)
        forward(d, 1)
        shared(d - 1)
        first = attend(d - 1, 0, first)
        forward(d, 2)
        forward(d, 3)
        second = attend(d - 1, 1, second)
    shared(4)
    first, second = attend(4, 0, first), attend(4, 1, second)
    mass = jnp.concatenate([first[1], second[1]], axis=0)
    acc = jnp.concatenate([first[2], second[2]], axis=0)
    ob[...] = (acc / mass).astype(BF16).reshape(4, 64, HEAD)

    slot_o = links.slots(4)
    mine = slot_o + lax.rem(x, 2) * 2 + c
    cols = pl.ds(pl.multiple_of(128 * lax.rem(x, 2), 128), 128)
    for dx in range(1, NX):
        tx = xat(dx)
        links.start(ob.at[tx], outb.at[half_rows, cols], (z, tx, y, x // 2), mine)
    stays = c == x // 2
    to_partner = links.copy(ob.at[x], outb.at[half_rows, cols], partner, mine, 3)

    @pl.when(stays)
    def _():
        outb[half_rows, cols] = ob[x]

    @pl.when(jnp.logical_not(stays))
    def _():
        to_partner.start()

    for k in range(4):
        from_me = stays & (lax.rem(x, 2) * 2 + c == k)

        @pl.when(jnp.logical_not(from_me))
        def _():
            links.wait(outb.at[half_rows, cols], slot_o + k, partner)

    out_ref[...] = outb[...]

    @pl.when(jnp.logical_not(stays))
    def _():
        to_partner.wait_send()

    for send in range(2):
        assert links.sent[send] % 16384 == 0
        links.drain(send, bx.at[0 : links.sent[send] // 2048], partner)
    links.drain(2, ids.at[0, :, 0:384], partner)
    links.drain(4, ss.at[0:3], partner)
    links.drain(7, r3.at[1:8], partner)
    links.drain(8, r2.at[0:3, :, 0:1664], partner)
    links.drain(5, sz, partner)
    links.drain(6, ids.at[0:4], partner)
    assert links.recvs <= RECVS, links.recvs


SENDS, RECVS = 9, 72
SEND_MOST = 4 << 20


def body(
    mixer_input, gate_input, document_ids, residual, select_weight, step_weight, step_bias, decay_log, skip_gain,
    out_weight, norm_gain, project_weight,
):
    vmem = pl.BlockSpec(memory_space=pltpu.VMEM)
    hbm = pl.BlockSpec(memory_space=pltpu.HBM)
    operands = (
        mixer_input,
        gate_input,
        document_ids.reshape(1, 128),
        residual,
        select_weight.T,
        step_weight,
        step_bias.reshape(1, 512),
        decay_log.T,
        skip_gain.reshape(1, 512),
        out_weight.T,
        norm_gain.reshape(1, 2048),
        project_weight.transpose(1, 0, 2),
    )
    scratch = [pltpu.VMEM(o.shape, o.dtype) for o in operands]
    scratch += [
        pltpu.VMEM((160, 128), BF16),
        pltpu.VMEM((160, 128), BF16),
        pltpu.VMEM((4, 160, 128), BF16),
        pltpu.VMEM((1, 128), F32),
        pltpu.VMEM((2, 32, 384), BF16),
        pltpu.VMEM((5, 1, 512), F32),
        pltpu.VMEM((128, 512), F32),
        pltpu.VMEM((2048, 512), F32),
        pltpu.VMEM((2048, 512), BF16),
        pltpu.VMEM((4, 16, 512), BF16),
        pltpu.VMEM((4, 1, 512), F32),
        pltpu.VMEM((4, 16, 512), BF16),
        pltpu.VMEM((4, 1, 512), F32),
        pltpu.VMEM((16, 512), BF16),
        pltpu.VMEM((1, 512), F32),
        pltpu.VMEM((16, 4, 32, 512), BF16),
        pltpu.VMEM((16, 4, 32, 384), BF16),
        pltpu.VMEM((128, 512), F32),
        pltpu.VMEM((128, 512), BF16),
        pltpu.VMEM((64, 2048), BF16),
        pltpu.VMEM((64, 2048), BF16),
        pltpu.VMEM((128, 2048), F32),
        pltpu.VMEM((64, 2048), BF16),
        pltpu.VMEM((4, 16, 2048), BF16),
        pltpu.VMEM((128, 384), BF16),
        pltpu.VMEM((128, 384), F32),
        pltpu.VMEM((8, 16, 384), BF16),
        pltpu.VMEM((4, 4, 16, 1024), BF16),
        pltpu.VMEM((4, 4, 16, 1024), BF16),
        pltpu.VMEM((5, 4, 2, 64, 256), BF16),
        pltpu.VMEM((4, 128, 128), F32),
        pltpu.VMEM((4, 64, 128), BF16),
        pltpu.VMEM((128, 256), BF16),
        pltpu.SemaphoreType.DMA((12,)),
        pltpu.SemaphoreType.DMA((SENDS,)),
        pltpu.SemaphoreType.DMA((RECVS,)),
    ]
    return pl.pallas_call(
        kernel,
        out_shape=jax.ShapeDtypeStruct((128, 256), BF16),
        in_specs=[hbm] * len(operands),
        out_specs=vmem,
        scratch_shapes=scratch,
        compiler_params=pltpu.CompilerParams(collective_id=0, has_side_effects=True, vmem_limit_bytes=48 << 20),
    )(*[pltpu.with_memory_space_constraint(o, pltpu.HBM) for o in operands])


def solution(mesh):
    split = Mesh(mesh.devices.reshape(NZ, NX, NY, NC), ("z", "x", "y", "c"))
    placed = (
        P(SEQ, TP), P(SEQ, TP), P(SEQ), P(SEQ, None), P(TP, None), P(None, TP), P(TP), P(TP, None), P(TP),
        P(TP, SEQ), P(), P(SEQ, None, TP),
    )
    return jax.shard_map(body, mesh=split, in_specs=placed, out_specs=P(SEQ, TP), check_vma=False)
```

```python
import math

import jax
import jax.numpy as jnp
from jax import lax
from jax.experimental import pallas as pl
from jax.experimental.pallas import tpu as pltpu
from jax.sharding import Mesh
from jax.sharding import PartitionSpec as P

MESH = pl.DeviceIdType.MESH
NZ, NX, NY, NC = 16, 4, 4, 2
STATE = 16
RANK = 128
HEAD = 128
WINDOW = 2048
EPS = 1e-05
LOG2E = 1.4426950408889634
RESET = 1e6
HIDDEN = -1e30
SEQ = ("z", "x")
TP = ("y", "c")
F32 = jnp.float32
BF16 = jnp.bfloat16


def nt(a, b):
    return lax.dot_general(a, b, (((1,), (1,)), ((), ())), preferred_element_type=F32)


def nn(a, b):
    return jnp.dot(a, b, preferred_element_type=F32)


def iota(shape, dim):
    return lax.broadcasted_iota(jnp.int32, shape, dim)


def softplus(v):
    e = jnp.exp(-jnp.abs(v))
    small = e * (1.0 - e * (0.5 - e * (1.0 / 3.0 - e * 0.25)))
    return jnp.maximum(v, 0.0) + jnp.where(e < 0.01, small, jnp.log(1.0 + e))


class Links:
    def __init__(self, send, recv):
        self.send, self.recv = send, recv
        self.recvs = 0
        self.sent = [0] * SENDS

    def slots(self, count):
        first = self.recvs
        self.recvs += count
        return first

    def copy(self, src, dst, device, slot, send):
        return pltpu.make_async_remote_copy(
            src_ref=src,
            dst_ref=dst,
            send_sem=self.send.at[send],
            recv_sem=self.recv.at[slot],
            device_id=device,
            device_id_type=MESH,
        )

    def start(self, src, dst, device, slot, send=None):
        size = math.prod(src.shape) * jnp.dtype(src.dtype).itemsize
        if send is None:
            send = 0 if self.sent[0] + size <= SEND_MOST else 1
        self.sent[send] += size
        self.copy(src, dst, device, slot, send).start()

    def wait(self, dst, slot, device):
        self.copy(dst, dst, device, slot, 0).wait_recv()

    def drain(self, send, whole, device):
        self.copy(whole, whole, device, 0, send).wait_send()


def kernel(
    *refs
):
    homes, refs = refs[:12], refs[12:]
    out_ref, refs = refs[0], refs[1:]
    staged, refs = refs[:12], refs[12:]
    x_ref, g_ref, doc_ref, res_ref, sel_ref, stepw_ref, bias_ref, a_ref, skip_ref, wo_ref, gain_ref, proj_ref = staged
    (
        part, part2, parts, ids_ref, wp_ref, ids, dt2, bx, hb, hs, ss, hz, sz, hr, sr, xw, wp, ys, gt, ps, pr, pf, r2s, r2, st, p3, f3, r3, na, nb,
        kv, qd, ob, outb, local_sem, send_sem, recv_sem,
    ) = refs
    z, x, y, c = (lax.axis_index(n) for n in ("z", "x", "y", "c"))
    other = 1 - c

    def zat(d):
        return lax.rem(z + d + NZ, NZ)

    def xat(d):
        return lax.rem(x + d + NX, NX)

    def yat(d):
        return lax.rem(y + d, NY)

    def cat(d):
        return other if d else c

    peers = [(z, x, yat(dy), cat(dc)) for dy in range(NY) for dc in range(NC) if dy or dc]
    row_peers = [(z, xat(dx), y, cat(dc)) for dx in range(1, NX) for dc in range(NC)]
    far = [(zat(d), x, y, c) for d in (-4, -3, -2, -1, 1, 2, 3, 4)]
    barrier = pltpu.get_barrier_semaphore()
    everyone = peers + row_peers + far
    for device in everyone:
        pl.semaphore_signal(barrier, inc=1, device_id=device, device_id_type=MESH)

    links = Links(send_sem, recv_sem)
    groups = [[0, -1, 1, -2, 2], [-3, 3, -4, 4], [-5, 5, -6, 6], [-7, 7, 8]]

    def columns(d):
        return pl.ds(pl.multiple_of(128 * zat(-d), 128), 128)

    loads = [pltpu.make_async_copy(src, dst, local_sem.at[n]) for n, (src, dst) in enumerate(zip(homes, staged))]
    early = (0, 4, 2, 9, 11)
    late = (5, 6, 7, 8, 1, 3, 10)
    for n in early + late:
        loads[n].start()
    partner = (z, x, y, other)
    my_rows = pl.multiple_of(64 * c + 16 * y, 16)

    for n in early:
        loads[n].wait()
    ids_ref[...] = doc_ref[...].astype(F32)
    for hh in range(2):
        for j in range(3):
            wp_ref[hh, :, HEAD * j : HEAD * j + HEAD] = proj_ref[j, :, HEAD * hh : HEAD * hh + HEAD]
    part[0:128] = nt(x_ref[...], sel_ref[0:RANK]).astype(BF16)
    part[128:160] = nt(sel_ref[RANK:], x_ref[...]).astype(BF16)
    xw[z, x] = wo_ref[...]
    ids[0, :, pl.ds(pl.multiple_of(128 * x, 128), 128)] = ids_ref[...]
    r2[:, :, 1664:] = jnp.zeros((4, 16, 384), BF16)
    pl.semaphore_wait(barrier, len(everyone))

    slot_pair, slot_rs = links.slots(1), links.slots(1)
    links.start(part, parts.at[0], partner, slot_pair)

    slot_i1 = links.slots(1)
    row_part = pl.ds(pl.multiple_of(128 * x, 128), 128)
    for dx in range(1, NX):
        links.start(ids_ref, ids.at[0, :, row_part], (z, xat(dx), y, c), slot_i1, 2)
    slot_x0 = links.slots(1)
    for hh in range(2):
        links.start(wp_ref.at[hh], wp.at[z, x], (z, 2 * c + hh, y, 1 - x // 2), slot_x0)

    slot_wo, slot_wp = links.slots(8), links.slots(4)
    ringed = pl.ds(pl.multiple_of(2 * other, 2), 2)

    def ring_out(phase):
        for near in (2, 1):
            for sign in (1, -1):
                block = zat(-sign * 2 * (phase - 1))
                if sign * (2 * (phase - 1) + near) != -8:
                    links.start(
                        wo_ref if phase == 1 else xw.at[block, x],
                        xw.at[block, x],
                        (zat(sign * near), x, y, c),
                        slot_wo + 2 * phase - near,
                    )

    def ring_proj(phase):
        for sign in (1, -1):
            block = zat(-sign * 2 * (phase - 1))
            for near in (1, 2):
                far_by = sign * (2 * (phase - 1) + near)
                if far_by != -8:
                    links.start(
                        wp.at[block, ringed],
                        wp.at[block, ringed],
                        (zat(sign * near), x, y, c),
                        slot_wp + phase - 1,
                    )

    def ring_far(phase):
        links.wait(xw.at[0 : 2 - phase // 4, x], slot_wo + 2 * phase - 2, partner)

    def ring_near(phase):
        links.wait(xw.at[0:2, x], slot_wo + 2 * phase - 1, partner)

    def ring_proj_wait(phase):
        links.wait(wp.at[0 : 4 - phase // 4, ringed], slot_wp + phase - 1, partner)

    slot_near, slot_last = [links.slots(1) for _ in groups], [links.slots(1) for _ in range(2)]

    def spread(g, members):
        for d in members:
            piece = xw.at[zat(-d), x]
            for dx in (1, 3) if g < 2 else (2, 1, 3):
                links.start(piece, piece, (z, xat(dx), y, c), slot_near[g])

    def relay(g):
        links.wait(xw.at[0 : 2 * len(groups[g]), x], slot_near[g], partner)
        middle = (len(groups[g]) + 1) // 2
        for n, d in enumerate(groups[g]):
            toward = 1 if n < middle else -1
            piece = xw.at[zat(-d), xat(-toward)]
            links.start(piece, piece, (z, xat(toward), y, c), slot_last[g])

    def arrived(g):
        if g < 2:
            links.wait(xw.at[0 : len(groups[g]), x], slot_last[g], partner)
        else:
            links.wait(xw.at[0 : 3 * len(groups[g]), x], slot_near[g], partner)

    ring_out(1)
    spread(0, groups[0][:1])
    links.wait(parts.at[0], slot_pair, partner)
    selected = part[...].astype(F32) + parts[0].astype(F32)
    part2[...] = selected.astype(BF16)
    for dy in range(1, NY):
        links.start(part2, parts.at[dy], (z, x, yat(dy), c), slot_rs)
    for n in late:
        loads[n].wait()
    links.wait(ids.at[0, :, 0:384], slot_i1, partner)
    slot_i2 = links.slots(2)
    for dz in range(1, 5):
        links.start(ids.at[0], ids.at[dz], (zat(dz), x, y, c), slot_i2 + min(dz - 1, 1), 6)

    ring_far(1)
    ring_out(2)
    ring_near(1)
    spread(0, groups[0][1:])
    links.wait(wp.at[z, 0:2], slot_x0, partner)
    ring_proj(1)
    links.wait(parts.at[1:4], slot_rs, partner)
    for k in range(1, NY):
        selected = selected + parts[k].astype(F32)
    values = x_ref[...].astype(F32)
    step = softplus(nn(selected[:RANK].astype(BF16), stepw_ref[...]) + bias_ref[...])
    column = jnp.transpose(jnp.broadcast_to(ids_ref[...], (128, 128)))
    before = pltpu.roll(column, 1, axis=0)
    linked = (column == before) | (iota((128, 128), 0) == 0)
    for k in range(4):
        cols = slice(128 * k, 128 * k + 128)
        dt2[:, cols] = jnp.where(linked, step[:, cols], RESET)
    ss[x] = jnp.sum(dt2[...], axis=0, keepdims=True)
    slot_ss = links.slots(1)
    for dx in range(1, NX):
        links.start(ss.at[x], ss.at[x], (z, xat(dx), y, c), slot_ss, 4)

    driven = (step * values).astype(BF16)
    inputs = jnp.concatenate([selected[RANK : RANK + STATE]] * 16, axis=0)
    for k in range(8):
        token = iota((256, 128), 0) // STATE + k * 16
        spread_in = jnp.where(iota((256, 128), 1) == token, inputs, 0.0).astype(BF16)
        bx[256 * k : 256 * k + 256, :] = nn(spread_in, driven)
    rate = -jnp.exp(a_ref[...]) * LOG2E

    def scan(initial, keep_states):
        def advance(k, h):
            steps = dt2[pl.ds(pl.multiple_of(k * 8, 8), 8), :]
            for j in range(8):
                at = pl.ds(pl.multiple_of(k * 128 + j * 16, 16), 16)
                h = jnp.exp2(rate * steps[j : j + 1, :]) * h + bx[at, :]
                if keep_states:
                    hb[at, :] = h.astype(BF16)
            return h

        return lax.fori_loop(0, 16, advance, initial)

    hs[x] = scan(jnp.zeros((STATE, 512), F32), False).astype(BF16)
    slot_hs = links.slots(1)
    for dx in range(1, NX):
        links.start(hs.at[x], hs.at[x], (z, xat(dx), y, c), slot_hs)
    ring_far(2)
    ring_out(3)
    ring_near(2)
    spread(1, groups[1])
    relay(0)
    links.wait(ss.at[0:3], slot_ss, partner)
    links.wait(hs.at[0:3], slot_hs, partner)
    links.wait(ids.at[1], slot_i2, partner)
    prior = jnp.where(z == 0, -1.0, ids[1, :, 511:512])
    breaks = []
    for k in range(NX):
        if k:
            prior = ids[0, :, 128 * k - 1 : 128 * k]
        first = ids[0, :, 128 * k : 128 * k + 1]
        breaks.append(jnp.broadcast_to(jnp.where(first == prior, 0.0, RESET), (1, 512)))
    running = jnp.zeros((STATE, 512), F32)
    steps_sum = jnp.zeros((1, 512), F32)
    own_prior, own_steps, own_break = running, steps_sum, steps_sum
    for k in range(NX):
        own_prior = jnp.where(x == k, running, own_prior)
        own_steps = jnp.where(x == k, steps_sum, own_steps)
        own_break = jnp.where(x == k, breaks[k], own_break)
        steps_of = ss[k] + breaks[k]
        running = jnp.exp2(rate * steps_of) * running + hs[k].astype(F32)
        steps_sum = steps_sum + steps_of
    dt2[0:1, :] = dt2[0:1, :] + own_break
    hr[...] = running.astype(BF16)
    sr[...] = steps_sum
    slot_hz, slot_sz = links.slots(1), links.slots(1)
    for dz in range(1, 5):
        links.start(hr, hz.at[dz - 1], (zat(dz), x, y, c), slot_hz)
        links.start(sr, sz.at[dz - 1], (zat(dz), x, y, c), slot_sz, 5)
    ring_far(3)
    ring_out(4)
    ring_near(3)
    relay(1)
    spread(2, groups[2])
    ring_far(4)
    ring_near(4)
    spread(3, groups[3])
    links.wait(hz, slot_hz, partner)
    links.wait(sz, slot_sz, partner)
    above = jnp.zeros((STATE, 512), F32)
    for dz in range(4, 0, -1):
        joined = jnp.exp2(rate * sz[dz - 1]) * above + hz[dz - 1].astype(F32)
        above = jnp.where(z >= dz, joined, jnp.zeros_like(joined))
    carry = jnp.exp2(rate * own_steps) * above + own_prior
    ring_proj_wait(1)
    ring_proj(2)
    scan(carry, True)
    pick_out = (lax.rem(iota((STATE, 256), 1), STATE) == iota((STATE, 256), 0)).astype(BF16)
    coefs = lax.dot_general(
        selected[RANK + STATE :].astype(BF16), pick_out, (((0,), (0,)), ((), ())), preferred_element_type=F32
    )
    own_token = iota((16, 256), 1) // STATE == iota((16, 256), 0)

    for k in range(8):
        rows = slice(16 * k, 16 * k + 16)
        coef = jnp.where(own_token, coefs[rows], 0.0).astype(BF16)
        ys[rows, :] = nn(coef, hb[256 * k : 256 * k + 256, :])
    gate = g_ref[...].astype(F32)
    mixed = (ys[...] + skip_ref[...] * values) * (gate / (1.0 + jnp.exp(-gate)))
    gt[...] = mixed.astype(BF16)

    slot_pr = [links.slots(1) for _ in groups]
    slot_r2 = [links.slots(1) for _ in groups]
    half_rows = pl.ds(pl.multiple_of(64 * c, 64), 64)
    their_rows = pl.ds(pl.multiple_of(64 * other, 64), 64)

    def weight_of(d):
        return xw[zat(-d)].reshape(128, 512)

    starts = [128 * sum(len(before) for before in groups[:g]) for g in range(len(groups))]

    def span(g):
        return slice(starts[g], starts[g] + 128 * len(groups[g]))

    def project(g):
        for n, d in enumerate(groups[g]):
            at = starts[g] + 128 * n
            pf[:, at : at + 128] = nt(gt[...], weight_of(d))
        ps[:, span(g)] = pf[their_rows, span(g)].astype(BF16)
        links.start(ps.at[:, span(g)], pr.at[:, span(g)], partner, slot_pr[g])

    def finish(g):
        links.wait(pr.at[:, span(g)], slot_pr[g], partner)
        joined = pf[half_rows, span(g)] + pr[:, span(g)].astype(F32)
        pf[half_rows, span(g)] = joined
        r2s[:, span(g)] = joined.astype(BF16)
        for dy in range(1, NY):
            ty = yat(dy)
            piece = r2s.at[pl.ds(pl.multiple_of(16 * ty, 16), 16), span(g)]
            links.start(piece, r2.at[dy, :, span(g)], (z, x, ty, c), slot_r2[g], 8)

    arrived(0)
    project(0)
    arrived(1)
    project(1)
    finish(0)
    arrived(2)
    project(2)
    finish(1)
    ring_proj_wait(2)
    ring_proj(3)
    finish(2)
    arrived(3)
    slot_r3 = links.slots(1)
    for j, d in enumerate(groups[3]):
        product = nt(gt[...], weight_of(d))
        f3[:, 128 * j : 128 * j + 128] = product
        p3[:, 128 * j : 128 * j + 128] = product.astype(BF16)
    for dy in range(NY):
        for dc in range(NC):
            if dy or dc:
                ty, tc = yat(dy), cat(dc)
                rows = pl.ds(pl.multiple_of(64 * tc + 16 * ty, 16), 16)
                links.start(p3.at[rows], r3.at[dy * 2 + dc], (z, x, ty, tc), slot_r3, 7)
    for g in range(3):
        links.wait(r2.at[0:3, :, span(g)], slot_r2[g], partner)
    links.wait(r3.at[1:8], slot_r3, partner)
    straight = f3[pl.ds(my_rows, 16), :]
    for k in range(1, 8):
        straight = straight + r3[k].astype(F32)
    pf[pl.ds(my_rows, 16), span(3)] = straight
    stream = pf[pl.ds(my_rows, 16), :]
    for dy in range(1, NY):
        stream = stream + r2[dy].astype(F32)
    for n, d in enumerate(sum(groups, [])):
        st[:, columns(d)] = stream[:, 128 * n : 128 * n + 128]
    stream = st[...] + res_ref[pl.ds(my_rows, 16), :].astype(F32)
    links.wait(ids.at[2:5], slot_i2 + 1, partner)
    stream = stream.astype(BF16).astype(F32)
    normed = stream * lax.rsqrt(jnp.mean(stream * stream, axis=-1, keepdims=True) + EPS) * gain_ref[...]
    normed = normed.astype(BF16)

    na[x, y] = normed[:, :1024]
    nb[x, y] = normed[:, 1024:]
    slot_n1, slot_n2 = links.slots(3), links.slots(3)
    slot_n3, slot_n4 = links.slots(1), links.slots(1)
    for d in range(1, 4):
        links.start(na.at[x, y], na.at[x, y], (z, xat(d), y, c), slot_n1 + d - 1)
        links.start(nb.at[x, y], nb.at[x, y], (z, x, yat(d), c), slot_n2 + d - 1)

    def over_y(k):
        piece = na.at[xat(k), y]
        for d in range(1, 4):
            links.start(piece, piece, (z, x, yat(d), c), slot_n3)

    def over_x(k):
        piece = nb.at[x, yat(k)]
        for d in range(1, 4):
            links.start(piece, piece, (z, xat(d), y, c), slot_n4)

    over_y(0)
    over_x(0)
    ring_proj_wait(3)
    ring_proj(4)

    for k in range(NX):
        qd[k] = jnp.transpose(jnp.broadcast_to(ids[0, :, 128 * k : 128 * k + 128], (128, 128)))
    q_doc = jnp.concatenate([qd[k, half_rows, :] for k in range(NX)], axis=0)
    row_of = iota((256, 128), 0)
    in_row = 128 * (row_of // 64) + 64 * c + lax.rem(row_of, 64)
    for k in (3, 1, 2):
        links.wait(na.at[x, y], slot_n1 + 3 - k, partner)
        over_y(k)
        links.wait(nb.at[x, y], slot_n2 + 3 - k, partner)
        over_x(k)
    ring_proj_wait(4)
    slot_pw = links.slots(1)
    links.start(wp.at[:, ringed], wp.at[:, ringed], partner, slot_pw)

    slot_kz = [None] + [links.slots(4) for _ in range(4)]
    slot_kc = links.slots(5)

    def chunk(d, k, core):
        return kv.at[d, xat(k), core]

    def pass_on(d, k):
        if d < 4:
            links.start(chunk(d, k, c), chunk(d + 1, k, c), (zat(1), x, y, c), slot_kz[d + 1] + k)
        links.start(chunk(d, k, c), chunk(d, k, c), partner, slot_kc + d)

    def forward(d, k):
        links.wait(chunk(d, k, c), slot_kz[d] + k, partner)
        pass_on(d, k)

    links.wait(na.at[0:3], slot_n3, partner)
    links.wait(nb.at[0:3], slot_n4, partner)
    links.wait(wp.at[:, ringed], slot_pw, partner)
    made = nn(na[...].reshape(256, 1024), wp[0:8].reshape(1024, 384))
    made = made + nn(nb[...].reshape(256, 1024), wp[8:16].reshape(1024, 384))
    query = made[:, :HEAD].astype(BF16)
    kv[0, :, c] = made[:, HEAD:].astype(BF16).reshape(4, 64, 256)
    for k in range(4):
        pass_on(0, k)

    def attend(d, half, carried):
        top, mass, acc = carried
        rows = slice(128 * half, 128 * half + 128)
        scores = []
        for k in range(NX):
            piece = nt(query[rows], kv[d, k, :, :, :HEAD].reshape(128, HEAD)) * (HEAD**-0.5 * LOG2E)
            k_doc = jnp.where(z >= d, ids[d, :, 128 * k : 128 * k + 128], -1.0)
            allowed = jnp.broadcast_to(k_doc, (128, 128)) == q_doc[rows]
            ahead = iota((128, 128), 1) + 128 * k - in_row[rows]
            if d == 0:
                allowed = allowed & (ahead <= 0)
            if d == 4:
                allowed = allowed & (ahead > 0)
            scores.append(jnp.where(allowed, piece, HIDDEN))
        highest = jnp.maximum(jnp.maximum(scores[0], scores[1]), jnp.maximum(scores[2], scores[3]))
        new_top = jnp.maximum(top, jnp.max(highest, axis=-1, keepdims=True))
        shrink = jnp.exp2(top - new_top)
        probs = [jnp.exp2(piece - new_top) for piece in scores]
        added = (probs[0] + probs[1]) + (probs[2] + probs[3])
        mass = mass * shrink + jnp.sum(added, axis=-1, keepdims=True)
        joined = jnp.concatenate([p.astype(BF16) for p in probs], axis=1)
        acc = acc * shrink + nn(joined, kv[d, :, :, :, HEAD:].reshape(512, HEAD))
        return new_top, mass, acc

    def shared(d):
        links.wait(kv.at[d, :, other], slot_kc + d, partner)

    start = (jnp.full((128, 1), HIDDEN, F32), jnp.zeros((128, 1), F32), jnp.zeros((128, HEAD), F32))
    shared(0)
    first, second = attend(0, 0, start), attend(0, 1, start)
    for k in range(4):
        forward(1, k)
    for d in range(2, 5):
        forward(d, 0)
        forward(d, 1)
        shared(d - 1)
        first = attend(d - 1, 0, first)
        forward(d, 2)
        forward(d, 3)
        second = attend(d - 1, 1, second)
    shared(4)
    first, second = attend(4, 0, first), attend(4, 1, second)
    mass = jnp.concatenate([first[1], second[1]], axis=0)
    acc = jnp.concatenate([first[2], second[2]], axis=0)
    ob[...] = (acc / mass).astype(BF16).reshape(4, 64, HEAD)

    slot_o = links.slots(4)
    mine = slot_o + lax.rem(x, 2) * 2 + c
    cols = pl.ds(pl.multiple_of(128 * lax.rem(x, 2), 128), 128)
    for dx in range(1, NX):
        tx = xat(dx)
        links.start(ob.at[tx], outb.at[half_rows, cols], (z, tx, y, x // 2), mine)
    stays = c == x // 2
    to_partner = links.copy(ob.at[x], outb.at[half_rows, cols], partner, mine, 3)

    @pl.when(stays)
    def _():
        outb[half_rows, cols] = ob[x]

    @pl.when(jnp.logical_not(stays))
    def _():
        to_partner.start()

    for k in range(4):
        from_me = stays & (lax.rem(x, 2) * 2 + c == k)

        @pl.when(jnp.logical_not(from_me))
        def _():
            links.wait(outb.at[half_rows, cols], slot_o + k, partner)

    out_ref[...] = outb[...]

    @pl.when(jnp.logical_not(stays))
    def _():
        to_partner.wait_send()

    for send in range(2):
        assert links.sent[send] % 16384 == 0
        links.drain(send, bx.at[0 : links.sent[send] // 2048], partner)
    links.drain(2, ids.at[0, :, 0:384], partner)
    links.drain(4, ss.at[0:3], partner)
    links.drain(7, r3.at[1:8], partner)
    links.drain(8, r2.at[0:3, :, 0:1664], partner)
    links.drain(5, sz, partner)
    links.drain(6, ids.at[0:4], partner)
    assert links.recvs <= RECVS, links.recvs


SENDS, RECVS = 9, 72
SEND_MOST = 4 << 20


def body(
    mixer_input, gate_input, document_ids, residual, select_weight, step_weight, step_bias, decay_log, skip_gain,
    out_weight, norm_gain, project_weight,
):
    vmem = pl.BlockSpec(memory_space=pltpu.VMEM)
    hbm = pl.BlockSpec(memory_space=pltpu.HBM)
    operands = (
        mixer_input,
        gate_input,
        document_ids.reshape(1, 128),
        residual,
        select_weight.T,
        step_weight,
        step_bias.reshape(1, 512),
        decay_log.T,
        skip_gain.reshape(1, 512),
        out_weight.T,
        norm_gain.reshape(1, 2048),
        project_weight.transpose(1, 0, 2),
    )
    scratch = [pltpu.VMEM(o.shape, o.dtype) for o in operands]
    scratch += [
        pltpu.VMEM((160, 128), BF16),
        pltpu.VMEM((160, 128), BF16),
        pltpu.VMEM((4, 160, 128), BF16),
        pltpu.VMEM((1, 128), F32),
        pltpu.VMEM((2, 32, 384), BF16),
        pltpu.VMEM((5, 1, 512), F32),
        pltpu.VMEM((128, 512), F32),
        pltpu.VMEM((2048, 512), F32),
        pltpu.VMEM((2048, 512), BF16),
        pltpu.VMEM((4, 16, 512), BF16),
        pltpu.VMEM((4, 1, 512), F32),
        pltpu.VMEM((4, 16, 512), BF16),
        pltpu.VMEM((4, 1, 512), F32),
        pltpu.VMEM((16, 512), BF16),
        pltpu.VMEM((1, 512), F32),
        pltpu.VMEM((16, 4, 32, 512), BF16),
        pltpu.VMEM((16, 4, 32, 384), BF16),
        pltpu.VMEM((128, 512), F32),
        pltpu.VMEM((128, 512), BF16),
        pltpu.VMEM((64, 2048), BF16),
        pltpu.VMEM((64, 2048), BF16),
        pltpu.VMEM((128, 2048), F32),
        pltpu.VMEM((64, 2048), BF16),
        pltpu.VMEM((4, 16, 2048), BF16),
        pltpu.VMEM((16, 2048), F32),
        pltpu.VMEM((128, 384), BF16),
        pltpu.VMEM((128, 384), F32),
        pltpu.VMEM((8, 16, 384), BF16),
        pltpu.VMEM((4, 4, 16, 1024), BF16),
        pltpu.VMEM((4, 4, 16, 1024), BF16),
        pltpu.VMEM((5, 4, 2, 64, 256), BF16),
        pltpu.VMEM((4, 128, 128), F32),
        pltpu.VMEM((4, 64, 128), BF16),
        pltpu.VMEM((128, 256), BF16),
        pltpu.SemaphoreType.DMA((12,)),
        pltpu.SemaphoreType.DMA((SENDS,)),
        pltpu.SemaphoreType.DMA((RECVS,)),
    ]
    return pl.pallas_call(
        kernel,
        out_shape=jax.ShapeDtypeStruct((128, 256), BF16),
        in_specs=[hbm] * len(operands),
        out_specs=vmem,
        scratch_shapes=scratch,
        compiler_params=pltpu.CompilerParams(collective_id=0, has_side_effects=True, vmem_limit_bytes=48 << 20),
    )(*[pltpu.with_memory_space_constraint(o, pltpu.HBM) for o in operands])


def solution(mesh):
    split = Mesh(mesh.devices.reshape(NZ, NX, NY, NC), ("z", "x", "y", "c"))
    placed = (
        P(SEQ, TP), P(SEQ, TP), P(SEQ), P(SEQ, None), P(TP, None), P(None, TP), P(TP), P(TP, None), P(TP),
        P(TP, SEQ), P(), P(SEQ, None, TP),
    )
    return jax.shard_map(body, mesh=split, in_specs=placed, out_specs=P(SEQ, TP), check_vma=False)
```

```python
import math

import jax
import jax.numpy as jnp
from jax import lax
from jax.experimental import pallas as pl
from jax.experimental.pallas import tpu as pltpu
from jax.sharding import Mesh
from jax.sharding import PartitionSpec as P

MESH = pl.DeviceIdType.MESH
NZ, NX, NY, NC = 16, 4, 4, 2
STATE = 16
RANK = 128
HEAD = 128
WINDOW = 2048
EPS = 1e-05
LOG2E = 1.4426950408889634
RESET = 1e6
HIDDEN = -1e30
SEQ = ("z", "x")
TP = ("y", "c")
F32 = jnp.float32
BF16 = jnp.bfloat16


def nt(a, b):
    return lax.dot_general(a, b, (((1,), (1,)), ((), ())), preferred_element_type=F32)


def nn(a, b):
    return jnp.dot(a, b, preferred_element_type=F32)


def iota(shape, dim):
    return lax.broadcasted_iota(jnp.int32, shape, dim)


def softplus(v):
    e = jnp.exp(-jnp.abs(v))
    small = e * (1.0 - e * (0.5 - e * (1.0 / 3.0 - e * 0.25)))
    return jnp.maximum(v, 0.0) + jnp.where(e < 0.01, small, jnp.log(1.0 + e))


class Links:
    def __init__(self, send, recv):
        self.send, self.recv = send, recv
        self.recvs = 0
        self.sent = [0] * SENDS

    def slots(self, count):
        first = self.recvs
        self.recvs += count
        return first

    def copy(self, src, dst, device, slot, send):
        return pltpu.make_async_remote_copy(
            src_ref=src,
            dst_ref=dst,
            send_sem=self.send.at[send],
            recv_sem=self.recv.at[slot],
            device_id=device,
            device_id_type=MESH,
        )

    def start(self, src, dst, device, slot, send=None):
        size = math.prod(src.shape) * jnp.dtype(src.dtype).itemsize
        if send is None:
            send = 0 if self.sent[0] + size <= SEND_MOST else 1
        self.sent[send] += size
        self.copy(src, dst, device, slot, send).start()

    def wait(self, dst, slot, device):
        self.copy(dst, dst, device, slot, 0).wait_recv()

    def drain(self, send, whole, device):
        self.copy(whole, whole, device, 0, send).wait_send()


def kernel(
    *refs
):
    homes, refs = refs[:12], refs[12:]
    out_ref, refs = refs[0], refs[1:]
    staged, refs = refs[:12], refs[12:]
    x_ref, g_ref, doc_ref, res_ref, sel_ref, stepw_ref, bias_ref, a_ref, skip_ref, wo_ref, gain_ref, proj_ref = staged
    (
        part, part2, parts, ids_ref, wp_ref, ids, dt2, bx, hb, hs, ss, hz, sz, hr, sr, xw, wp, ys, gt, ps, pr, pf, r2s, r2, st, p3, f3, r3, na, nb,
        kv, qd, ob, outb, local_sem, send_sem, recv_sem,
    ) = refs
    z, x, y, c = (lax.axis_index(n) for n in ("z", "x", "y", "c"))
    other = 1 - c

    def zat(d):
        return lax.rem(z + d + NZ, NZ)

    def xat(d):
        return lax.rem(x + d + NX, NX)

    def yat(d):
        return lax.rem(y + d, NY)

    def cat(d):
        return other if d else c

    peers = [(z, x, yat(dy), cat(dc)) for dy in range(NY) for dc in range(NC) if dy or dc]
    row_peers = [(z, xat(dx), y, cat(dc)) for dx in range(1, NX) for dc in range(NC)]
    far = [(zat(d), x, y, c) for d in (-4, -3, -2, -1, 1, 2, 3, 4)]
    barrier = pltpu.get_barrier_semaphore()
    everyone = peers + row_peers + far
    for device in everyone:
        pl.semaphore_signal(barrier, inc=1, device_id=device, device_id_type=MESH)

    links = Links(send_sem, recv_sem)
    groups = [[0, -1, 1, -2, 2], [-3, 3, -4, 4], [-5, 5, -6, 6], [-7, 7, 8]]

    def columns(d):
        return pl.ds(pl.multiple_of(128 * zat(-d), 128), 128)

    loads = [pltpu.make_async_copy(src, dst, local_sem.at[n]) for n, (src, dst) in enumerate(zip(homes, staged))]
    early = (0, 4, 2, 9, 11)
    late = (5, 6, 7, 8, 1, 3, 10)
    for n in early + late:
        loads[n].start()
    partner = (z, x, y, other)
    my_rows = pl.multiple_of(64 * c + 16 * y, 16)

    for n in early:
        loads[n].wait()
    ids_ref[...] = doc_ref[...].astype(F32)
    for hh in range(2):
        for j in range(3):
            wp_ref[hh, :, HEAD * j : HEAD * j + HEAD] = proj_ref[j, :, HEAD * hh : HEAD * hh + HEAD]
    part[0:128] = nt(x_ref[...], sel_ref[0:RANK]).astype(BF16)
    part[128:160] = nt(sel_ref[RANK:], x_ref[...]).astype(BF16)
    xw[z, x] = wo_ref[...]
    ids[0, :, pl.ds(pl.multiple_of(128 * x, 128), 128)] = ids_ref[...]
    r2[:, :, 1664:] = jnp.zeros((4, 16, 384), BF16)
    pl.semaphore_wait(barrier, len(everyone))

    slot_pair, slot_rs = links.slots(1), links.slots(1)
    links.start(part, parts.at[0], partner, slot_pair)

    slot_i1 = links.slots(1)
    row_part = pl.ds(pl.multiple_of(128 * x, 128), 128)
    for dx in range(1, NX):
        links.start(ids_ref, ids.at[0, :, row_part], (z, xat(dx), y, c), slot_i1, 2)
    slot_x0 = links.slots(1)
    for hh in range(2):
        links.start(wp_ref.at[hh], wp.at[z, x], (z, 2 * c + hh, y, 1 - x // 2), slot_x0)

    slot_wo, slot_wp = links.slots(8), links.slots(4)
    ringed = pl.ds(pl.multiple_of(2 * other, 2), 2)

    def ring_out(phase):
        for near in (2, 1):
            for sign in (1, -1):
                block = zat(-sign * 2 * (phase - 1))
                if sign * (2 * (phase - 1) + near) != -8:
                    links.start(
                        wo_ref if phase == 1 else xw.at[block, x],
                        xw.at[block, x],
                        (zat(sign * near), x, y, c),
                        slot_wo + 2 * phase - near,
                    )

    def ring_proj(phase):
        for sign in (1, -1):
            block = zat(-sign * 2 * (phase - 1))
            for near in (1, 2):
                far_by = sign * (2 * (phase - 1) + near)
                if far_by != -8:
                    links.start(
                        wp.at[block, ringed],
                        wp.at[block, ringed],
                        (zat(sign * near), x, y, c),
                        slot_wp + phase - 1,
                    )

    def ring_far(phase):
        links.wait(xw.at[0 : 2 - phase // 4, x], slot_wo + 2 * phase - 2, partner)

    def ring_near(phase):
        links.wait(xw.at[0:2, x], slot_wo + 2 * phase - 1, partner)

    def ring_proj_wait(phase):
        links.wait(wp.at[0 : 4 - phase // 4, ringed], slot_wp + phase - 1, partner)

    slot_near, slot_last = [links.slots(1) for _ in groups], [links.slots(1) for _ in range(2)]

    def spread(g, members):
        for d in members:
            piece = xw.at[zat(-d), x]
            for dx in (1, 3) if g < 2 else (2, 1, 3):
                links.start(piece, piece, (z, xat(dx), y, c), slot_near[g])

    def relay(g):
        links.wait(xw.at[0 : 2 * len(groups[g]), x], slot_near[g], partner)
        middle = (len(groups[g]) + 1) // 2
        for n, d in enumerate(groups[g]):
            toward = 1 if n < middle else -1
            piece = xw.at[zat(-d), xat(-toward)]
            links.start(piece, piece, (z, xat(toward), y, c), slot_last[g])

    def arrived(g):
        if g < 2:
            links.wait(xw.at[0 : len(groups[g]), x], slot_last[g], partner)
        else:
            links.wait(xw.at[0 : 3 * len(groups[g]), x], slot_near[g], partner)

    ring_out(1)
    spread(0, groups[0][:1])
    links.wait(parts.at[0], slot_pair, partner)
    selected = part[...].astype(F32) + parts[0].astype(F32)
    part2[...] = selected.astype(BF16)
    for dy in range(1, NY):
        links.start(part2, parts.at[dy], (z, x, yat(dy), c), slot_rs)
    for n in late:
        loads[n].wait()
    links.wait(ids.at[0, :, 0:384], slot_i1, partner)
    slot_i2 = links.slots(2)
    for dz in range(1, 5):
        links.start(ids.at[0], ids.at[dz], (zat(dz), x, y, c), slot_i2 + min(dz - 1, 1), 6)

    ring_far(1)
    ring_out(2)
    ring_near(1)
    spread(0, groups[0][1:])
    links.wait(wp.at[z, 0:2], slot_x0, partner)
    ring_proj(1)
    links.wait(parts.at[1:4], slot_rs, partner)
    for k in range(1, NY):
        selected = selected + parts[k].astype(F32)
    values = x_ref[...].astype(F32)
    step = softplus(nn(selected[:RANK].astype(BF16), stepw_ref[...]) + bias_ref[...])
    column = jnp.transpose(jnp.broadcast_to(ids_ref[...], (128, 128)))
    before = pltpu.roll(column, 1, axis=0)
    linked = (column == before) | (iota((128, 128), 0) == 0)
    for k in range(4):
        cols = slice(128 * k, 128 * k + 128)
        dt2[:, cols] = jnp.where(linked, step[:, cols], RESET)
    ss[x] = jnp.sum(dt2[...], axis=0, keepdims=True)
    slot_ss = links.slots(1)
    for dx in range(1, NX):
        links.start(ss.at[x], ss.at[x], (z, xat(dx), y, c), slot_ss, 4)

    driven = (step * values).astype(BF16)
    inputs = jnp.concatenate([selected[RANK : RANK + STATE]] * 16, axis=0)
    for k in range(8):
        token = iota((256, 128), 0) // STATE + k * 16
        spread_in = jnp.where(iota((256, 128), 1) == token, inputs, 0.0).astype(BF16)
        bx[256 * k : 256 * k + 256, :] = nn(spread_in, driven)
    rate = -jnp.exp(a_ref[...]) * LOG2E

    def scan(initial, keep_states):
        def advance(k, h):
            steps = dt2[pl.ds(pl.multiple_of(k * 8, 8), 8), :]
            for j in range(8):
                at = pl.ds(pl.multiple_of(k * 128 + j * 16, 16), 16)
                h = jnp.exp2(rate * steps[j : j + 1, :]) * h + bx[at, :]
                if keep_states:
                    hb[at, :] = h.astype(BF16)
            return h

        return lax.fori_loop(0, 16, advance, initial)

    hs[x] = scan(jnp.zeros((STATE, 512), F32), False).astype(BF16)
    slot_hs = links.slots(1)
    for dx in range(1, NX):
        links.start(hs.at[x], hs.at[x], (z, xat(dx), y, c), slot_hs)
    ring_far(2)
    ring_out(3)
    ring_near(2)
    spread(1, groups[1])
    relay(0)
    links.wait(ss.at[0:3], slot_ss, partner)
    links.wait(hs.at[0:3], slot_hs, partner)
    links.wait(ids.at[1], slot_i2, partner)
    prior = jnp.where(z == 0, -1.0, ids[1, :, 511:512])
    breaks = []
    for k in range(NX):
        if k:
            prior = ids[0, :, 128 * k - 1 : 128 * k]
        first = ids[0, :, 128 * k : 128 * k + 1]
        breaks.append(jnp.broadcast_to(jnp.where(first == prior, 0.0, RESET), (1, 512)))
    running = jnp.zeros((STATE, 512), F32)
    steps_sum = jnp.zeros((1, 512), F32)
    own_prior, own_steps, own_break = running, steps_sum, steps_sum
    for k in range(NX):
        own_prior = jnp.where(x == k, running, own_prior)
        own_steps = jnp.where(x == k, steps_sum, own_steps)
        own_break = jnp.where(x == k, breaks[k], own_break)
        steps_of = ss[k] + breaks[k]
        running = jnp.exp2(rate * steps_of) * running + hs[k].astype(F32)
        steps_sum = steps_sum + steps_of
    dt2[0:1, :] = dt2[0:1, :] + own_break
    hr[...] = running.astype(BF16)
    sr[...] = steps_sum
    slot_hz, slot_sz = links.slots(1), links.slots(1)
    for dz in range(1, 5):
        links.start(hr, hz.at[dz - 1], (zat(dz), x, y, c), slot_hz)
        links.start(sr, sz.at[dz - 1], (zat(dz), x, y, c), slot_sz, 5)
    ring_far(3)
    ring_out(4)
    ring_near(3)
    relay(1)
    spread(2, groups[2])
    ring_far(4)
    ring_near(4)
    spread(3, groups[3])
    links.wait(hz, slot_hz, partner)
    links.wait(sz, slot_sz, partner)
    above = jnp.zeros((STATE, 512), F32)
    for dz in range(4, 0, -1):
        joined = jnp.exp2(rate * sz[dz - 1]) * above + hz[dz - 1].astype(F32)
        above = jnp.where(z >= dz, joined, jnp.zeros_like(joined))
    carry = jnp.exp2(rate * own_steps) * above + own_prior
    ring_proj_wait(1)
    ring_proj(2)
    scan(carry, True)
    pick_out = (lax.rem(iota((STATE, 256), 1), STATE) == iota((STATE, 256), 0)).astype(BF16)
    coefs = lax.dot_general(
        selected[RANK + STATE :].astype(BF16), pick_out, (((0,), (0,)), ((), ())), preferred_element_type=F32
    )
    own_token = iota((16, 256), 1) // STATE == iota((16, 256), 0)

    for k in range(8):
        rows = slice(16 * k, 16 * k + 16)
        coef = jnp.where(own_token, coefs[rows], 0.0).astype(BF16)
        ys[rows, :] = nn(coef, hb[256 * k : 256 * k + 256, :])
    gate = g_ref[...].astype(F32)
    mixed = (ys[...] + skip_ref[...] * values) * (gate / (1.0 + jnp.exp(-gate)))
    gt[...] = mixed.astype(BF16)

    slot_pr = [links.slots(1) for _ in groups]
    slot_r2 = [links.slots(1) for _ in groups]
    half_rows = pl.ds(pl.multiple_of(64 * c, 64), 64)
    their_rows = pl.ds(pl.multiple_of(64 * other, 64), 64)

    def weight_of(d):
        return xw[zat(-d)].reshape(128, 512)

    starts = [128 * sum(len(before) for before in groups[:g]) for g in range(len(groups))]

    def span(g):
        return slice(starts[g], starts[g] + 128 * len(groups[g]))

    def project(g):
        for n, d in enumerate(groups[g]):
            at = starts[g] + 128 * n
            pf[:, at : at + 128] = nt(gt[...], weight_of(d))
        ps[:, span(g)] = pf[their_rows, span(g)].astype(BF16)
        links.start(ps.at[:, span(g)], pr.at[:, span(g)], partner, slot_pr[g])

    def finish(g):
        links.wait(pr.at[:, span(g)], slot_pr[g], partner)
        joined = pf[half_rows, span(g)] + pr[:, span(g)].astype(F32)
        pf[half_rows, span(g)] = joined
        r2s[:, span(g)] = joined.astype(BF16)
        for dy in range(1, NY):
            ty = yat(dy)
            piece = r2s.at[pl.ds(pl.multiple_of(16 * ty, 16), 16), span(g)]
            links.start(piece, r2.at[dy, :, span(g)], (z, x, ty, c), slot_r2[g], 8)

    arrived(0)
    project(0)
    arrived(1)
    project(1)
    finish(0)
    arrived(2)
    project(2)
    finish(1)
    finish(2)
    ring_proj_wait(2)
    ring_proj(3)
    arrived(3)
    slot_r3 = links.slots(1)
    for j, d in enumerate(groups[3]):
        product = nt(gt[...], weight_of(d))
        f3[:, 128 * j : 128 * j + 128] = product
        p3[:, 128 * j : 128 * j + 128] = product.astype(BF16)
    for dy in range(NY):
        for dc in range(NC):
            if dy or dc:
                ty, tc = yat(dy), cat(dc)
                rows = pl.ds(pl.multiple_of(64 * tc + 16 * ty, 16), 16)
                links.start(p3.at[rows], r3.at[dy * 2 + dc], (z, x, ty, tc), slot_r3, 7)
    for g in range(3):
        links.wait(r2.at[0:3, :, span(g)], slot_r2[g], partner)
    links.wait(r3.at[1:8], slot_r3, partner)
    straight = f3[pl.ds(my_rows, 16), :]
    for k in range(1, 8):
        straight = straight + r3[k].astype(F32)
    pf[pl.ds(my_rows, 16), span(3)] = straight
    stream = pf[pl.ds(my_rows, 16), :]
    for dy in range(1, NY):
        stream = stream + r2[dy].astype(F32)
    for n, d in enumerate(sum(groups, [])):
        st[:, columns(d)] = stream[:, 128 * n : 128 * n + 128]
    stream = st[...] + res_ref[pl.ds(my_rows, 16), :].astype(F32)
    links.wait(ids.at[2:5], slot_i2 + 1, partner)
    stream = stream.astype(BF16).astype(F32)
    normed = stream * lax.rsqrt(jnp.mean(stream * stream, axis=-1, keepdims=True) + EPS) * gain_ref[...]
    normed = normed.astype(BF16)

    na[x, y] = normed[:, :1024]
    nb[x, y] = normed[:, 1024:]
    slot_n1, slot_n2 = links.slots(3), links.slots(3)
    slot_n3, slot_n4 = links.slots(1), links.slots(1)
    for d in range(1, 4):
        links.start(na.at[x, y], na.at[x, y], (z, xat(d), y, c), slot_n1 + d - 1)
        links.start(nb.at[x, y], nb.at[x, y], (z, x, yat(d), c), slot_n2 + d - 1)

    def over_y(k):
        piece = na.at[xat(k), y]
        for d in range(1, 4):
            links.start(piece, piece, (z, x, yat(d), c), slot_n3)

    def over_x(k):
        piece = nb.at[x, yat(k)]
        for d in range(1, 4):
            links.start(piece, piece, (z, xat(d), y, c), slot_n4)

    over_y(0)
    over_x(0)
    ring_proj_wait(3)
    ring_proj(4)

    for k in range(NX):
        qd[k] = jnp.transpose(jnp.broadcast_to(ids[0, :, 128 * k : 128 * k + 128], (128, 128)))
    q_doc = jnp.concatenate([qd[k, half_rows, :] for k in range(NX)], axis=0)
    row_of = iota((256, 128), 0)
    in_row = 128 * (row_of // 64) + 64 * c + lax.rem(row_of, 64)
    for k in (3, 1, 2):
        links.wait(na.at[x, y], slot_n1 + 3 - k, partner)
        over_y(k)
        links.wait(nb.at[x, y], slot_n2 + 3 - k, partner)
        over_x(k)
    ring_proj_wait(4)
    slot_pw = links.slots(1)
    links.start(wp.at[:, ringed], wp.at[:, ringed], partner, slot_pw)

    slot_kz = [None] + [links.slots(4) for _ in range(4)]
    slot_kc = links.slots(5)

    def chunk(d, k, core):
        return kv.at[d, xat(k), core]

    def pass_on(d, k):
        if d < 4:
            links.start(chunk(d, k, c), chunk(d + 1, k, c), (zat(1), x, y, c), slot_kz[d + 1] + k)
        links.start(chunk(d, k, c), chunk(d, k, c), partner, slot_kc + d)

    def forward(d, k):
        links.wait(chunk(d, k, c), slot_kz[d] + k, partner)
        pass_on(d, k)

    links.wait(na.at[0:3], slot_n3, partner)
    links.wait(nb.at[0:3], slot_n4, partner)
    links.wait(wp.at[:, ringed], slot_pw, partner)
    made = nn(na[...].reshape(256, 1024), wp[0:8].reshape(1024, 384))
    made = made + nn(nb[...].reshape(256, 1024), wp[8:16].reshape(1024, 384))
    query = made[:, :HEAD].astype(BF16)
    kv[0, :, c] = made[:, HEAD:].astype(BF16).reshape(4, 64, 256)
    for k in range(4):
        pass_on(0, k)

    def attend(d, half, carried):
        top, mass, acc = carried
        rows = slice(128 * half, 128 * half + 128)
        scores = []
        for k in range(NX):
            piece = nt(query[rows], kv[d, k, :, :, :HEAD].reshape(128, HEAD)) * (HEAD**-0.5 * LOG2E)
            k_doc = jnp.where(z >= d, ids[d, :, 128 * k : 128 * k + 128], -1.0)
            allowed = jnp.broadcast_to(k_doc, (128, 128)) == q_doc[rows]
            ahead = iota((128, 128), 1) + 128 * k - in_row[rows]
            if d == 0:
                allowed = allowed & (ahead <= 0)
            if d == 4:
                allowed = allowed & (ahead > 0)
            scores.append(jnp.where(allowed, piece, HIDDEN))
        highest = jnp.maximum(jnp.maximum(scores[0], scores[1]), jnp.maximum(scores[2], scores[3]))
        new_top = jnp.maximum(top, jnp.max(highest, axis=-1, keepdims=True))
        shrink = jnp.exp2(top - new_top)
        probs = [jnp.exp2(piece - new_top) for piece in scores]
        added = (probs[0] + probs[1]) + (probs[2] + probs[3])
        mass = mass * shrink + jnp.sum(added, axis=-1, keepdims=True)
        joined = jnp.concatenate([p.astype(BF16) for p in probs], axis=1)
        acc = acc * shrink + nn(joined, kv[d, :, :, :, HEAD:].reshape(512, HEAD))
        return new_top, mass, acc

    def shared(d):
        links.wait(kv.at[d, :, other], slot_kc + d, partner)

    start = (jnp.full((128, 1), HIDDEN, F32), jnp.zeros((128, 1), F32), jnp.zeros((128, HEAD), F32))
    shared(0)
    first, second = attend(0, 0, start), attend(0, 1, start)
    for k in range(4):
        forward(1, k)
    for d in range(2, 5):
        forward(d, 0)
        forward(d, 1)
        shared(d - 1)
        first = attend(d - 1, 0, first)
        forward(d, 2)
        forward(d, 3)
        second = attend(d - 1, 1, second)
    shared(4)
    first, second = attend(4, 0, first), attend(4, 1, second)
    mass = jnp.concatenate([first[1], second[1]], axis=0)
    acc = jnp.concatenate([first[2], second[2]], axis=0)
    ob[...] = (acc / mass).astype(BF16).reshape(4, 64, HEAD)

    slot_o = links.slots(4)
    mine = slot_o + lax.rem(x, 2) * 2 + c
    cols = pl.ds(pl.multiple_of(128 * lax.rem(x, 2), 128), 128)
    for dx in range(1, NX):
        tx = xat(dx)
        links.start(ob.at[tx], outb.at[half_rows, cols], (z, tx, y, x // 2), mine)
    stays = c == x // 2
    to_partner = links.copy(ob.at[x], outb.at[half_rows, cols], partner, mine, 3)

    @pl.when(stays)
    def _():
        outb[half_rows, cols] = ob[x]

    @pl.when(jnp.logical_not(stays))
    def _():
        to_partner.start()

    for k in range(4):
        from_me = stays & (lax.rem(x, 2) * 2 + c == k)

        @pl.when(jnp.logical_not(from_me))
        def _():
            links.wait(outb.at[half_rows, cols], slot_o + k, partner)

    out_ref[...] = outb[...]

    @pl.when(jnp.logical_not(stays))
    def _():
        to_partner.wait_send()

    for send in range(2):
        assert links.sent[send] % 16384 == 0
        links.drain(send, bx.at[0 : links.sent[send] // 2048], partner)
    links.drain(2, ids.at[0, :, 0:384], partner)
    links.drain(4, ss.at[0:3], partner)
    links.drain(7, r3.at[1:8], partner)
    links.drain(8, r2.at[0:3, :, 0:1664], partner)
    links.drain(5, sz, partner)
    links.drain(6, ids.at[0:4], partner)
    assert links.recvs <= RECVS, links.recvs


SENDS, RECVS = 9, 72
SEND_MOST = 4 << 20


def body(
    mixer_input, gate_input, document_ids, residual, select_weight, step_weight, step_bias, decay_log, skip_gain,
    out_weight, norm_gain, project_weight,
):
    vmem = pl.BlockSpec(memory_space=pltpu.VMEM)
    hbm = pl.BlockSpec(memory_space=pltpu.HBM)
    operands = (
        mixer_input,
        gate_input,
        document_ids.reshape(1, 128),
        residual,
        select_weight.T,
        step_weight,
        step_bias.reshape(1, 512),
        decay_log.T,
        skip_gain.reshape(1, 512),
        out_weight.T,
        norm_gain.reshape(1, 2048),
        project_weight.transpose(1, 0, 2),
    )
    scratch = [pltpu.VMEM(o.shape, o.dtype) for o in operands]
    scratch += [
        pltpu.VMEM((160, 128), BF16),
        pltpu.VMEM((160, 128), BF16),
        pltpu.VMEM((4, 160, 128), BF16),
        pltpu.VMEM((1, 128), F32),
        pltpu.VMEM((2, 32, 384), BF16),
        pltpu.VMEM((5, 1, 512), F32),
        pltpu.VMEM((128, 512), F32),
        pltpu.VMEM((2048, 512), F32),
        pltpu.VMEM((2048, 512), BF16),
        pltpu.VMEM((4, 16, 512), BF16),
        pltpu.VMEM((4, 1, 512), F32),
        pltpu.VMEM((4, 16, 512), BF16),
        pltpu.VMEM((4, 1, 512), F32),
        pltpu.VMEM((16, 512), BF16),
        pltpu.VMEM((1, 512), F32),
        pltpu.VMEM((16, 4, 32, 512), BF16),
        pltpu.VMEM((16, 4, 32, 384), BF16),
        pltpu.VMEM((128, 512), F32),
        pltpu.VMEM((128, 512), BF16),
        pltpu.VMEM((64, 2048), BF16),
        pltpu.VMEM((64, 2048), BF16),
        pltpu.VMEM((128, 2048), F32),
        pltpu.VMEM((64, 2048), BF16),
        pltpu.VMEM((4, 16, 2048), BF16),
        pltpu.VMEM((16, 2048), F32),
        pltpu.VMEM((128, 384), BF16),
        pltpu.VMEM((128, 384), F32),
        pltpu.VMEM((8, 16, 384), BF16),
        pltpu.VMEM((4, 4, 16, 1024), BF16),
        pltpu.VMEM((4, 4, 16, 1024), BF16),
        pltpu.VMEM((5, 4, 2, 64, 256), BF16),
        pltpu.VMEM((4, 128, 128), F32),
        pltpu.VMEM((4, 64, 128), BF16),
        pltpu.VMEM((128, 256), BF16),
        pltpu.SemaphoreType.DMA((12,)),
        pltpu.SemaphoreType.DMA((SENDS,)),
        pltpu.SemaphoreType.DMA((RECVS,)),
    ]
    return pl.pallas_call(
        kernel,
        out_shape=jax.ShapeDtypeStruct((128, 256), BF16),
        in_specs=[hbm] * len(operands),
        out_specs=vmem,
        scratch_shapes=scratch,
        compiler_params=pltpu.CompilerParams(collective_id=0, has_side_effects=True, vmem_limit_bytes=48 << 20),
    )(*[pltpu.with_memory_space_constraint(o, pltpu.HBM) for o in operands])


def solution(mesh):
    split = Mesh(mesh.devices.reshape(NZ, NX, NY, NC), ("z", "x", "y", "c"))
    placed = (
        P(SEQ, TP), P(SEQ, TP), P(SEQ), P(SEQ, None), P(TP, None), P(None, TP), P(TP), P(TP, None), P(TP),
        P(TP, SEQ), P(), P(SEQ, None, TP),
    )
    return jax.shard_map(body, mesh=split, in_specs=placed, out_specs=P(SEQ, TP), check_vma=False)
```
